32 devices in a mesh: member: 4 (over y, x), space: 8 (over z, core).
Axes of the slice: x: 2, y: 2, z: 4, core: 2. Of those that a mesh axis runs over, the one named last changes fastest.
Arguments:
- ensemble: float32 [128, 16, 16, 128], P(None, 'space', 'member'), may hold values from -4 to 4
- source: float32 [16, 16, 128], P('space', 'member'), may hold values from -6 to 6
- obs_rows: int32 [8, 4, 1], P('space', 'member'), may hold values from 0 to 7
- obs_values: float32 [8, 4, 128], P('space', 'member'), may hold values from -3 to 3
- obs_noise: float32 [128, 8, 4, 128], P(None, 'space', 'member'), may hold values from -5 to 5
- obs_var: float32 [8, 4, 128], P('space', 'member'), may hold values from 0.05 to 2
Outputs:
- updated: float32 [128, 16, 16, 128], P(None, 'space', 'member')
- predicted: float32 [128, 8, 4, 128], P(None, 'space', 'member')
The draws below stay inside these ranges and needn't reach their ends.
Inputs may be any that keep to these rules, and one draw needn't show every extreme that they name: `obs_rows`: entry [s, m, o] names the cell row at (s * 2 + r // 4, m * 4 + r % 4) of the first two dimensions, whose 128 cells along the third dimension are observed; rows may repeat.
All inputs are finite; a program needn't handle non-finite values.
Results may differ from the reference program's by a relative error of at most 0.0003.
Values sent between devices are 32-bit elements; how exact they have to be, the bound alone decides.
No kernel may reach another device: no remote copies, remote signals or barrier semaphores. Data moves between devices by JAX's collectives and lax.ppermute only.
A program may use at most 64 MiB of HBM per device.

```python
import math
import jax
import jax.numpy as jnp
from jax import lax

M = 128
CX = 2
CY = 4
NZ = 128
OBS_DEV = 1
ITERS = 4
NX = 16
NY = 16
N_MEMBER = 4
N_SPACE = 8


def with_ends(drawn, key, least, largest):
    index_at = [jax.random.randint(jax.random.fold_in(key, axis), (), 0, length) for axis, length in enumerate(drawn.shape)]
    longest = drawn.shape.index(max(drawn.shape))
    next_to = index_at[:longest] + [(index_at[longest] + 1) % drawn.shape[longest]] + index_at[longest + 1:]
    return drawn.at[tuple(index_at)].set(least).at[tuple(next_to)].set(largest)


def levels(key, shape, split, smallest, top_value):
    loudness, own = 1.0, jax.random.fold_in(key, 6)
    for dim, blocks in split:
        draws = jnp.exp(jax.random.uniform(jax.random.fold_in(own, dim), (blocks,), jnp.float32, smallest / len(split), top_value / len(split)))
        loudness = loudness * jnp.repeat(draws, shape[dim] // blocks).reshape([-1 if axis == dim else 1 for axis in range(len(shape))])
    return loudness


def centred(stream_key, dims, scale, bound, cuts=(), kind=jnp.bfloat16):
    array = scale * jax.random.normal(stream_key, dims, jnp.float32)
    if cuts:
        array = array * levels(stream_key, dims, cuts, -0.22, 0.18)
    return jnp.clip(array, -bound, bound).astype(kind)


def setup_inputs(seed: int = 0) -> dict:
    arg_keys = jax.random.split(jax.random.key(seed), 7)
    ensemble = centred(arg_keys[0], (M, NX, NY, NZ), 1.0, 4.0, ((1, 8), (2, 4)), jnp.float32)
    source = centred(arg_keys[1], (NX, NY, NZ), 1.0, 6.0, ((0, 8), (1, 4)), jnp.float32)
    obs_rows = with_ends(jax.random.randint(arg_keys[2], (N_SPACE, N_MEMBER, OBS_DEV), 0, CX * CY), jax.random.fold_in(arg_keys[2], 1), 0, (CX * CY) - 1).astype(jnp.int32)
    obs_values = centred(arg_keys[3], (N_SPACE, N_MEMBER, OBS_DEV * NZ), 0.5, 3.0, ((0, 8), (1, 4)), jnp.float32)
    obs_noise = centred(arg_keys[4], (M, N_SPACE, N_MEMBER, OBS_DEV * NZ), 1.0, 5.0, ((1, 8), (2, 4)), jnp.float32)
    obs_var = jnp.clip(jnp.exp(math.log(2.0) - 3.6888794 * jax.random.uniform(arg_keys[5], (N_SPACE, N_MEMBER, OBS_DEV * NZ), jnp.float32) ** levels(arg_keys[5], (N_SPACE, N_MEMBER, OBS_DEV * NZ), ((0, 8), (1, 4)), -0.2, 0.2)), 0.05, 2.0)
    return {"ensemble": ensemble, "source": source, "obs_rows": obs_rows, "obs_values": obs_values, "obs_noise": obs_noise, "obs_var": obs_var}


def harmonic(first_cond, second_cond):
    return 2.0 * first_cond * second_cond / (first_cond + second_cond)

def face_terms(cond):
    cond_pad = jnp.pad(cond, 1, mode='edge')
    face_x = harmonic(cond_pad[:-1, 1:-1, 1:-1], cond_pad[1:, 1:-1, 1:-1])
    face_y = harmonic(cond_pad[1:-1, :-1, 1:-1], cond_pad[1:-1, 1:, 1:-1])
    face_z = harmonic(cond, cond_pad[1:-1, 1:-1, 2:])
    lower_z = jnp.concatenate([harmonic(cond[..., :1], cond[..., :1]), face_z[..., :-1]], axis=-1)
    return (face_x, face_y, face_z, lower_z)

def operate(values_in, face_x, face_y, face_z, lower_z):
    padded = jnp.pad(values_in, 1)
    result = face_x[1:] * (values_in - padded[2:, 1:-1, 1:-1]) + face_x[:-1] * (values_in - padded[:-2, 1:-1, 1:-1])
    result = result + face_y[:, 1:] * (values_in - padded[1:-1, 2:, 1:-1]) + face_y[:, :-1] * (values_in - padded[1:-1, :-2, 1:-1])
    result = result + face_z * (values_in - padded[1:-1, 1:-1, 2:]) + lower_z * (values_in - padded[1:-1, 1:-1, :-2])
    return result

def conjugate(cond, source):
    face_x, face_y, face_z, lower_z = face_terms(cond)
    residual = source
    direction = source
    solution = jnp.zeros_like(source)
    norm_now = jnp.sum(residual * residual)
    for iteration in range(ITERS):
        image = operate(direction, face_x, face_y, face_z, lower_z)
        step_size = norm_now / jnp.sum(direction * image)
        solution = solution + step_size * direction
        residual = residual - step_size * image
        if iteration + 1 < ITERS:
            norm_next = jnp.sum(residual * residual)
            direction = residual + norm_next / norm_now * direction
            norm_now = norm_next
    return solution

def reference(ensemble, source, obs_rows, obs_values, obs_noise, obs_var):
    slab_ids = jnp.arange(N_SPACE).astype(jnp.int32)[:, None, None]
    column_ids = jnp.arange(N_MEMBER).astype(jnp.int32)[None, :, None]
    cell_x = slab_ids * CX + obs_rows // CY
    cell_y = column_ids * CY + obs_rows % CY

    def member_pred(member_field):
        pressure = conjugate(jnp.exp(member_field), source)
        return pressure[cell_x, cell_y, :].reshape(N_SPACE, N_MEMBER, OBS_DEV * NZ)
    predicted = lax.map(member_pred, ensemble)
    flat_pred = predicted.reshape(M, -1)
    inv_sigma = 1.0 / jnp.sqrt(obs_var.reshape(-1))
    spread = (flat_pred - lax.optimization_barrier(jnp.mean(flat_pred, axis=0))) * inv_sigma
    misfit = (obs_values.reshape(-1) - flat_pred) * inv_sigma + obs_noise.reshape(M, -1)
    gram_sum = jnp.dot(spread, spread.T, precision=lax.Precision.HIGHEST)
    cross_sum = jnp.dot(spread, misfit.T, precision=lax.Precision.HIGHEST)
    factor = jnp.linalg.cholesky(gram_sum + (M - 1.0) * jnp.eye(M, dtype=jnp.float32))
    weights = jax.scipy.linalg.cho_solve((factor, True), cross_sum)
    flat_field = ensemble.reshape(M, -1)
    anomalies = flat_field - lax.optimization_barrier(jnp.mean(flat_field, axis=0))
    updated = flat_field + jnp.dot(weights.T, anomalies, precision=lax.Precision.HIGHEST)
    return (updated.reshape(ensemble.shape), predicted)
```

```python
import functools

import jax
import jax.numpy as jnp
from jax import lax
from jax.experimental import pallas as pl
from jax.experimental.pallas import tpu as pltpu
from jax.sharding import PartitionSpec as P

ITERS = 4
AXES = ("member", "space")
HIGHEST = lax.Precision.HIGHEST


def padded_2(x, sides, width):
    for axis, dim in sides:
        devices, length = (lax.axis_size(axis), x.shape[dim])
        up = [(i, (i + 1) % devices) for i in range(devices - 1)]
        down = [(j, i) for i, j in up]
        last = lax.slice_in_dim(x, length - width, length, axis=dim)
        leading = lax.slice_in_dim(x, 0, width, axis=dim)
        before = lax.ppermute(last, axis, up)
        after = lax.ppermute(leading, axis, down)
        x = jnp.concatenate([before, x, after], axis=dim)
    return x


def harmonic(first_cond, second_cond):
    return 2.0 * first_cond * second_cond / (first_cond + second_cond)


def extend(values_in):
    widened = padded_2(values_in, (("member", 2),), 1)
    return jnp.pad(widened, ((0, 0), (1, 1), (0, 0), (1, 1)))


def member_dots(dot_terms):
    return lax.psum(dot_terms, "member")


def face_terms(cond):
    widened = extend(cond)
    edge_pad = jnp.pad(cond, ((0, 0), (1, 1), (1, 1), (1, 1)), mode="edge")
    cond_pad = jnp.where(widened > 0.0, widened, edge_pad)
    face_x = harmonic(cond_pad[:, :-1, 1:-1, 1:-1], cond_pad[:, 1:, 1:-1, 1:-1])
    face_y = harmonic(cond_pad[:, 1:-1, :-1, 1:-1], cond_pad[:, 1:-1, 1:, 1:-1])
    face_z = harmonic(cond, cond_pad[:, 1:-1, 1:-1, 2:])
    lower_z = jnp.concatenate([harmonic(cond[..., :1], cond[..., :1]), face_z[..., :-1]], axis=-1)
    return (face_x, face_y, face_z, lower_z)


def operate(values_in, face_x, face_y, face_z, lower_z):
    padded = extend(values_in)
    result = face_x[:, 1:] * (values_in - padded[:, 2:, 1:-1, 1:-1]) + face_x[:, :-1] * (
        values_in - padded[:, :-2, 1:-1, 1:-1]
    )
    result = (
        result
        + face_y[:, :, 1:] * (values_in - padded[:, 1:-1, 2:, 1:-1])
        + face_y[:, :, :-1] * (values_in - padded[:, 1:-1, :-2, 1:-1])
    )
    result = (
        result
        + face_z * (values_in - padded[:, 1:-1, 1:-1, 2:])
        + lower_z * (values_in - padded[:, 1:-1, 1:-1, :-2])
    )
    return result


def conjugate(cond, forcing):
    face_x, face_y, face_z, lower_z = face_terms(cond)
    residual = jnp.broadcast_to(forcing[None], cond.shape)
    direction = residual
    solution = jnp.zeros_like(cond)
    norm_now = member_dots(jnp.sum(residual * residual, axis=(1, 2, 3)))
    for iteration in range(ITERS):
        image = operate(direction, face_x, face_y, face_z, lower_z)
        step_size = norm_now / member_dots(jnp.sum(direction * image, axis=(1, 2, 3)))
        solution = solution + step_size[:, None, None, None] * direction
        residual = residual - step_size[:, None, None, None] * image
        if iteration + 1 < ITERS:
            norm_next = member_dots(jnp.sum(residual * residual, axis=(1, 2, 3)))
            direction = residual + (norm_next / norm_now)[:, None, None, None] * direction
            norm_now = norm_next
    return solution


def local_split(ensemble, source, obs_rows, obs_values, obs_noise, obs_var):
    total_members = ensemble.shape[0]
    block_x, block_y, layers = source.shape
    held_fields = lax.all_to_all(ensemble, "space", split_axis=0, concat_axis=1, tiled=True)
    forcing = lax.all_gather(source, "space", axis=0, tiled=True)
    pressure = conjugate(jnp.exp(held_fields), forcing)
    held_count = pressure.shape[0]
    cells_flat = pressure.reshape(held_count, -1, layers)
    gathered_rows = lax.all_gather(obs_rows, "space", axis=0, tiled=True)
    row_ids = gathered_rows[:, 0]
    peer_ids = jnp.arange(row_ids.shape[0], dtype=jnp.int32)[:, None]
    flat_index = (peer_ids * block_x + row_ids // block_y) * block_y + row_ids % block_y
    picked = jnp.take(cells_flat, flat_index.reshape(-1), axis=1)
    returned = lax.all_to_all(picked, "space", split_axis=1, concat_axis=0, tiled=True)
    predicted = returned.reshape(total_members, 1, 1, -1)
    flat_pred = returned.reshape(total_members, -1)
    inv_sigma = 1.0 / jnp.sqrt(obs_var.reshape(-1))
    spread = (flat_pred - jnp.mean(flat_pred, axis=0)) * inv_sigma
    misfit = (obs_values.reshape(-1) - flat_pred) * inv_sigma + obs_noise.reshape(total_members, -1)
    gram_part = jnp.dot(spread, spread.T, precision=HIGHEST)
    cross_part = jnp.dot(spread, misfit.T, precision=HIGHEST)
    gram_sum, cross_sum = lax.psum((gram_part, cross_part), AXES)
    factor = jnp.linalg.cholesky(
        gram_sum + (total_members - 1.0) * jnp.eye(total_members, dtype=jnp.float32)
    )
    weights = jax.scipy.linalg.cho_solve((factor, True), cross_sum)
    flat_field = ensemble.reshape(total_members, -1)
    anomalies = flat_field - jnp.mean(flat_field, axis=0)
    updated = flat_field + jnp.dot(weights.T, anomalies, precision=HIGHEST)
    return (updated.reshape(ensemble.shape), predicted)


def vmem_call(kernel, out_shape, scratch, name, *operands):
    spec = pl.BlockSpec(memory_space=pltpu.VMEM)
    return pl.pallas_call(
        kernel,
        out_shape=jax.ShapeDtypeStruct(out_shape, jnp.float32),
        in_specs=[spec] * len(operands),
        out_specs=spec,
        scratch_shapes=[pltpu.VMEM(s, jnp.float32) for s in scratch],
        name=name,
    )(*operands)


def total(acc):
    return jnp.sum(jnp.sum(acc, axis=0, keepdims=True), axis=1, keepdims=True)


def pressure_kernel(g_ref, out_ref, e_ref, fx_ref, fy_ref, fz_ref, bd_ref, p_ref, r_ref, q_ref, x_ref, *, dims):
    n_m, n_s, held, bx, by, n_obs = dims
    nx, ny = n_s * bx, n_m * by
    nz = g_ref.shape[1]
    block = bx * by
    rows = (held + 1) * block + n_obs
    lane = lax.broadcasted_iota(jnp.int32, (ny, nz), 1)
    sub = lax.broadcasted_iota(jnp.int32, (ny, nz), 0)

    def at(j, x):
        start = (j * nx + x) * ny
        return pl.ds(start, ny)

    def here(ref, j, x):
        return ref[at(j, x), :]

    for m in range(n_m):
        for s in range(n_s):
            base = (m * n_s + s) * rows
            for a in range(bx):
                x = s * bx + a
                for j in range(held):
                    e_ref[pl.ds((j * nx + x) * ny + m * by, by), :] = g_ref[
                        pl.ds(base + j * block + a * by, by), :
                    ]
                x_ref[pl.ds(x * ny + m * by, by), :] = g_ref[pl.ds(base + held * block + a * by, by), :]

    edge_z = (lane == 0).astype(jnp.float32) + (lane == nz - 1).astype(jnp.float32)
    edge_y = (sub == 0).astype(jnp.float32) + (sub == ny - 1).astype(jnp.float32)
    inner_z = lane > 0
    inner_y = sub > 0
    norm0 = jnp.zeros((ny, nz), jnp.float32)
    for x in range(nx):
        v = here(x_ref, 0, x)
        norm0 = norm0 + v * v
        for j in range(held):
            p_ref[at(j, x), :] = v
            r_ref[at(j, x), :] = v
    norm_now = [total(norm0)] * held

    for j in range(held):
        before = None
        for x in range(nx):
            e = jnp.exp(-here(e_ref, j, x))
            if before is not None:
                fx_ref[at(j, x), :] = 2.0 / (e + before)
            fy_ref[at(j, x), :] = jnp.where(inner_y, 2.0 / (e + pltpu.roll(e, 1, 0)), 0.0)
            fz_ref[at(j, x), :] = jnp.where(inner_z, 2.0 / (e + pltpu.roll(e, 1, 1)), 0.0)
            ends = edge_y + edge_z
            if x == 0 or x == nx - 1:
                ends = ends + 1.0
            bd_ref[at(j, x), :] = ends / e
            before = e

    for iteration in range(ITERS):
        last = iteration + 1 == ITERS
        steps = []
        for j in range(held):
            acc = jnp.zeros((ny, nz), jnp.float32)
            v = here(p_ref, j, 0)
            gx = None
            for x in range(nx):
                gy = here(fy_ref, j, x) * (v - pltpu.roll(v, 1, 0))
                gz = here(fz_ref, j, x) * (v - pltpu.roll(v, 1, 1))
                image = here(bd_ref, j, x) * v
                image = image + (gy - pltpu.roll(gy, ny - 1, 0))
                image = image + (gz - pltpu.roll(gz, nz - 1, 1))
                if gx is not None:
                    image = image + gx
                if x + 1 < nx:
                    after = here(p_ref, j, x + 1)
                    gx = here(fx_ref, j, x + 1) * (after - v)
                    image = image - gx
                if not last:
                    q_ref[at(j, x), :] = image
                acc = acc + v * image
                if x + 1 < nx:
                    v = after
            steps.append(norm_now[j] / total(acc))
        norm_next = []
        for j in range(held):
            step = jnp.broadcast_to(steps[j], (ny, nz))
            acc = jnp.zeros((ny, nz), jnp.float32)
            for x in range(nx):
                add = step * here(p_ref, j, x)
                x_ref[at(j, x), :] = add if iteration == 0 else here(x_ref, j, x) + add
                if not last:
                    res = here(r_ref, j, x) - step * here(q_ref, j, x)
                    r_ref[at(j, x), :] = res
                    acc = acc + res * res
            if not last:
                norm_next.append(total(acc))
        if not last:
            for j in range(held):
                ratio = jnp.broadcast_to(norm_next[j] / norm_now[j], (ny, nz))
                for x in range(nx):
                    p_ref[at(j, x), :] = here(r_ref, j, x) + ratio * here(p_ref, j, x)
            norm_now = norm_next

    for m in range(n_m):
        for s in range(n_s):
            peer = m * n_s + s
            for o in range(n_obs):
                picked = g_ref[pl.ds(peer * rows + (held + 1) * block + o, 1), :].astype(jnp.int32)[0, 0]
                cell = (s * bx + picked // by) * ny + m * by + picked % by
                for j in range(held):
                    out_ref[pl.ds((peer * held + j) * n_obs + o, 1), :] = x_ref[pl.ds(j * nx * ny + cell, 1), :]


def sums_kernel(pred_ref, values_ref, noise_ref, var_ref, out_ref, *, devices):
    members = pred_ref.shape[0]
    held = members // devices
    pred = pred_ref[...]
    inv_sigma = 1.0 / jnp.sqrt(var_ref[...])
    mean = jnp.sum(pred, axis=0, keepdims=True) / members
    spread = (pred - mean) * inv_sigma
    misfit = (values_ref[...] - pred) * inv_sigma + noise_ref[...]
    by_last = (((1,), (1,)), ((), ()))
    gram = lax.dot_general(spread, spread, by_last, precision=HIGHEST, preferred_element_type=jnp.float32)
    cross = lax.dot_general(spread, misfit, by_last, precision=HIGHEST, preferred_element_type=jnp.float32)
    for d in range(devices):
        out_ref[d, 0:held, :] = gram[d * held : (d + 1) * held, :]
        out_ref[d, held : 2 * held, :] = cross[d * held : (d + 1) * held, :]


def update_kernel(sums_ref, field_ref, out_ref, a_ref, c_ref, *, devices):
    members = sums_ref.shape[2]
    held = members // devices
    tile = 8
    for d in range(devices):
        a_ref[pl.ds(d * held, held), :] = sums_ref[d, 0:held, :]
        c_ref[pl.ds(d * held, held), :] = sums_ref[d, held : 2 * held, :]
    lane = lax.broadcasted_iota(jnp.int32, (tile, members), 1)
    sub = lax.broadcasted_iota(jnp.int32, (tile, members), 0)
    blocks = members // tile
    left, right = [], []
    for k in range(blocks):
        own = (lane == sub + k * tile).astype(jnp.float32) * (members - 1.0)
        left.append(a_ref[pl.ds(k * tile, tile), :] + own)
        right.append(c_ref[pl.ds(k * tile, tile), :])
    wide = (tile, members)

    def row(x, t):
        return jnp.broadcast_to(x[t : t + 1, :], wide)

    def column(x, t):
        return jnp.broadcast_to(x[:, t : t + 1], wide)

    for k in range(blocks):
        parts = [column(left[k], k * tile + t) for t in range(tile)] + [left[k], right[k]]
        for t in range(tile):
            inverse = 1.0 / row(parts[t], t)
            factor = jnp.where(sub == t, 0.0, parts[t] * inverse)
            scaled = sub == t
            for i in range(t + 1, len(parts)):
                pivot = row(parts[i], t)
                parts[i] = jnp.where(scaled, pivot * inverse, parts[i] - factor * pivot)
        left[k], right[k] = parts[-2], parts[-1]
        rows_left = [row(left[k], t) for t in range(tile)]
        rows_right = [row(right[k], t) for t in range(tile)]
        for i in range(blocks):
            if i != k:
                columns = [column(left[i], k * tile + t) for t in range(tile)]
                for t in range(tile):
                    right[i] = right[i] - columns[t] * rows_right[t]
                    if k + 1 < blocks:
                        left[i] = left[i] - columns[t] * rows_left[t]
    for k in range(blocks):
        c_ref[pl.ds(k * tile, tile), :] = right[k]
    weights = c_ref[...]
    cells = field_ref.shape[0] // members
    by_first = (((0,), (0,)), ((), ()))
    for c in range(cells):
        field = field_ref[pl.ds(c, members, stride=cells), :]
        anomaly = field - jnp.sum(field, axis=0, keepdims=True) / members
        moved = lax.dot_general(weights, anomaly, by_first, precision=HIGHEST, preferred_element_type=jnp.float32)
        out_ref[pl.ds(c, members, stride=cells), :] = field + moved


def exchange(x):
    return lax.all_to_all(x, AXES, split_axis=0, concat_axis=0, tiled=True)


def local_whole(ensemble, source, obs_rows, obs_values, obs_noise, obs_var):
    members = ensemble.shape[0]
    bx, by, nz = source.shape
    n_m, n_s = lax.axis_size("member"), lax.axis_size("space")
    devices = n_m * n_s
    held = members // devices
    block = bx * by
    n_obs = obs_rows.shape[-1]
    wide = (devices, block, 1, nz)
    packed = jnp.concatenate(
        [
            ensemble.reshape(devices, held * block, 1, nz),
            jnp.broadcast_to(source.reshape(1, block, 1, nz), wide),
            jnp.broadcast_to(obs_rows.astype(jnp.float32).reshape(1, n_obs, 1, 1), (devices, n_obs, 1, nz)),
        ],
        axis=1,
    )
    rows = packed.shape[1]
    got = exchange(packed.reshape(devices * rows, 1, nz)).reshape(devices * rows, nz)
    nx, ny = n_s * bx, n_m * by
    field = (held * nx * ny, nz)
    picked = vmem_call(
        functools.partial(pressure_kernel, dims=(n_m, n_s, held, bx, by, n_obs)),
        (members * n_obs, nz),
        [field] * 9,
        "pressure",
        got,
    )
    returned = exchange(picked.reshape(members * n_obs, 1, nz))
    sums = vmem_call(
        functools.partial(sums_kernel, devices=devices),
        (devices, 2 * held, members),
        [],
        "sums",
        returned.reshape(members, n_obs * nz),
        obs_values.reshape(1, -1),
        obs_noise.reshape(members, -1),
        obs_var.reshape(1, -1),
    )
    own = jnp.sum(exchange(sums), axis=0, keepdims=True)
    gathered = exchange(jnp.broadcast_to(own, sums.shape))
    updated = vmem_call(
        functools.partial(update_kernel, devices=devices),
        (members * block, nz),
        [(members, members)] * 2,
        "update",
        gathered,
        ensemble.reshape(members * block, nz),
    )
    return (updated.reshape(ensemble.shape), returned.reshape(members, 1, 1, n_obs * nz))


def local(ensemble, *rest):
    devices = lax.axis_size("member") * lax.axis_size("space")
    form = local_whole if ensemble.shape[0] % devices == 0 else local_split
    return form(ensemble, *rest)


def solution(mesh):
    in_specs = (
        P(None, "space", "member", None),
        P("space", "member", None),
        P("space", "member", None),
        P("space", "member", None),
        P(None, "space", "member", None),
        P("space", "member", None),
    )
    out_specs = (P(None, "space", "member", None), P(None, "space", "member", None))
    return jax.shard_map(local, mesh=mesh, in_specs=in_specs, out_specs=out_specs, check_vma=False)
```

```python
import functools

import jax
import jax.numpy as jnp
from jax import lax
from jax.experimental import pallas as pl
from jax.experimental.pallas import tpu as pltpu
from jax.sharding import PartitionSpec as P

ITERS = 4
AXES = ("member", "space")
HIGHEST = lax.Precision.HIGHEST


def padded_2(x, sides, width):
    for axis, dim in sides:
        devices, length = (lax.axis_size(axis), x.shape[dim])
        up = [(i, (i + 1) % devices) for i in range(devices - 1)]
        down = [(j, i) for i, j in up]
        last = lax.slice_in_dim(x, length - width, length, axis=dim)
        leading = lax.slice_in_dim(x, 0, width, axis=dim)
        before = lax.ppermute(last, axis, up)
        after = lax.ppermute(leading, axis, down)
        x = jnp.concatenate([before, x, after], axis=dim)
    return x


def harmonic(first_cond, second_cond):
    return 2.0 * first_cond * second_cond / (first_cond + second_cond)


def extend(values_in):
    widened = padded_2(values_in, (("member", 2),), 1)
    return jnp.pad(widened, ((0, 0), (1, 1), (0, 0), (1, 1)))


def member_dots(dot_terms):
    return lax.psum(dot_terms, "member")


def face_terms(cond):
    widened = extend(cond)
    edge_pad = jnp.pad(cond, ((0, 0), (1, 1), (1, 1), (1, 1)), mode="edge")
    cond_pad = jnp.where(widened > 0.0, widened, edge_pad)
    face_x = harmonic(cond_pad[:, :-1, 1:-1, 1:-1], cond_pad[:, 1:, 1:-1, 1:-1])
    face_y = harmonic(cond_pad[:, 1:-1, :-1, 1:-1], cond_pad[:, 1:-1, 1:, 1:-1])
    face_z = harmonic(cond, cond_pad[:, 1:-1, 1:-1, 2:])
    lower_z = jnp.concatenate([harmonic(cond[..., :1], cond[..., :1]), face_z[..., :-1]], axis=-1)
    return (face_x, face_y, face_z, lower_z)


def operate(values_in, face_x, face_y, face_z, lower_z):
    padded = extend(values_in)
    result = face_x[:, 1:] * (values_in - padded[:, 2:, 1:-1, 1:-1]) + face_x[:, :-1] * (
        values_in - padded[:, :-2, 1:-1, 1:-1]
    )
    result = (
        result
        + face_y[:, :, 1:] * (values_in - padded[:, 1:-1, 2:, 1:-1])
        + face_y[:, :, :-1] * (values_in - padded[:, 1:-1, :-2, 1:-1])
    )
    result = (
        result
        + face_z * (values_in - padded[:, 1:-1, 1:-1, 2:])
        + lower_z * (values_in - padded[:, 1:-1, 1:-1, :-2])
    )
    return result


def conjugate(cond, forcing):
    face_x, face_y, face_z, lower_z = face_terms(cond)
    residual = jnp.broadcast_to(forcing[None], cond.shape)
    direction = residual
    solution = jnp.zeros_like(cond)
    norm_now = member_dots(jnp.sum(residual * residual, axis=(1, 2, 3)))
    for iteration in range(ITERS):
        image = operate(direction, face_x, face_y, face_z, lower_z)
        step_size = norm_now / member_dots(jnp.sum(direction * image, axis=(1, 2, 3)))
        solution = solution + step_size[:, None, None, None] * direction
        residual = residual - step_size[:, None, None, None] * image
        if iteration + 1 < ITERS:
            norm_next = member_dots(jnp.sum(residual * residual, axis=(1, 2, 3)))
            direction = residual + (norm_next / norm_now)[:, None, None, None] * direction
            norm_now = norm_next
    return solution


def local_split(ensemble, source, obs_rows, obs_values, obs_noise, obs_var):
    total_members = ensemble.shape[0]
    block_x, block_y, layers = source.shape
    held_fields = lax.all_to_all(ensemble, "space", split_axis=0, concat_axis=1, tiled=True)
    forcing = lax.all_gather(source, "space", axis=0, tiled=True)
    pressure = conjugate(jnp.exp(held_fields), forcing)
    held_count = pressure.shape[0]
    cells_flat = pressure.reshape(held_count, -1, layers)
    gathered_rows = lax.all_gather(obs_rows, "space", axis=0, tiled=True)
    row_ids = gathered_rows[:, 0]
    peer_ids = jnp.arange(row_ids.shape[0], dtype=jnp.int32)[:, None]
    flat_index = (peer_ids * block_x + row_ids // block_y) * block_y + row_ids % block_y
    picked = jnp.take(cells_flat, flat_index.reshape(-1), axis=1)
    returned = lax.all_to_all(picked, "space", split_axis=1, concat_axis=0, tiled=True)
    predicted = returned.reshape(total_members, 1, 1, -1)
    flat_pred = returned.reshape(total_members, -1)
    inv_sigma = 1.0 / jnp.sqrt(obs_var.reshape(-1))
    spread = (flat_pred - jnp.mean(flat_pred, axis=0)) * inv_sigma
    misfit = (obs_values.reshape(-1) - flat_pred) * inv_sigma + obs_noise.reshape(total_members, -1)
    gram_part = jnp.dot(spread, spread.T, precision=HIGHEST)
    cross_part = jnp.dot(spread, misfit.T, precision=HIGHEST)
    gram_sum, cross_sum = lax.psum((gram_part, cross_part), AXES)
    factor = jnp.linalg.cholesky(
        gram_sum + (total_members - 1.0) * jnp.eye(total_members, dtype=jnp.float32)
    )
    weights = jax.scipy.linalg.cho_solve((factor, True), cross_sum)
    flat_field = ensemble.reshape(total_members, -1)
    anomalies = flat_field - jnp.mean(flat_field, axis=0)
    updated = flat_field + jnp.dot(weights.T, anomalies, precision=HIGHEST)
    return (updated.reshape(ensemble.shape), predicted)


def vmem_call(kernel, out_shape, scratch, name, *operands):
    spec = pl.BlockSpec(memory_space=pltpu.VMEM)
    return pl.pallas_call(
        kernel,
        out_shape=jax.ShapeDtypeStruct(out_shape, jnp.float32),
        in_specs=[spec] * len(operands),
        out_specs=spec,
        scratch_shapes=[pltpu.VMEM(s, jnp.float32) for s in scratch],
        name=name,
    )(*operands)


def total(acc):
    return jnp.sum(jnp.sum(acc, axis=0, keepdims=True), axis=1, keepdims=True)


def pressure_kernel(g_ref, out_ref, e_ref, fx_ref, fy_ref, fz_ref, bd_ref, p_ref, r_ref, q_ref, x_ref, acc_ref, norm_ref, *, dims):
    n_m, n_s, held, bx, by, n_obs = dims
    nx, ny = n_s * bx, n_m * by
    nz = g_ref.shape[1]
    block = bx * by
    rows = (held + 1) * block + n_obs
    plane = (ny, nz)
    lane = lax.broadcasted_iota(jnp.int32, plane, 1)
    sub = lax.broadcasted_iota(jnp.int32, plane, 0)

    def at(j, x):
        return pl.ds(pl.multiple_of((j * nx + x) * ny, ny), ny)

    def member(j):
        return pl.ds(pl.multiple_of(j * ny, ny), ny)

    def for_members(fn):
        def body(j, carry):
            fn(j)
            return carry

        lax.fori_loop(0, held, body, 0)

    for m in range(n_m):
        for s in range(n_s):
            base = (m * n_s + s) * rows
            for a in range(bx):
                x = s * bx + a
                for j in range(held):
                    e_ref[pl.ds((j * nx + x) * ny + m * by, by), :] = g_ref[
                        pl.ds(base + j * block + a * by, by), :
                    ]
                x_ref[pl.ds(x * ny + m * by, by), :] = g_ref[pl.ds(base + held * block + a * by, by), :]

    edge_z = (lane == 0).astype(jnp.float32) + (lane == nz - 1).astype(jnp.float32)
    edge_y = (sub == 0).astype(jnp.float32) + (sub == ny - 1).astype(jnp.float32)
    norm0 = jnp.zeros(plane, jnp.float32)
    for x in range(nx):
        v = x_ref[at(0, x), :]
        norm0 = norm0 + v * v
        for j in range(held):
            p_ref[at(j, x), :] = v
            r_ref[at(j, x), :] = v
    norm0 = jnp.broadcast_to(total(norm0), plane)
    for j in range(held):
        norm_ref[member(j), :] = norm0

    def faces(j):
        before = None
        for x in range(nx):
            e = jnp.exp(-e_ref[at(j, x), :])
            if before is not None:
                fx_ref[at(j, x), :] = 2.0 / (e + before)
            fy_ref[at(j, x), :] = jnp.where(sub > 0, 2.0 / (e + pltpu.roll(e, 1, 0)), 0.0)
            fz_ref[at(j, x), :] = jnp.where(lane > 0, 2.0 / (e + pltpu.roll(e, 1, 1)), 0.0)
            ends = edge_y + edge_z
            if x == 0 or x == nx - 1:
                ends = ends + 1.0
            bd_ref[at(j, x), :] = ends / e
            before = e

    for_members(faces)

    def along_z(j):
        for x in range(nx):
            v = p_ref[at(j, x), :]
            gz = fz_ref[at(j, x), :] * (v - pltpu.roll(v, 1, 1))
            q_ref[at(j, x), :] = gz - pltpu.roll(gz, nz - 1, 1)

    def apply(j):
        acc = jnp.zeros(plane, jnp.float32)
        v = p_ref[at(j, 0), :]
        gx = None
        for x in range(nx):
            gy = fy_ref[at(j, x), :] * (v - pltpu.roll(v, 1, 0))
            image = q_ref[at(j, x), :] + bd_ref[at(j, x), :] * v
            image = image + (gy - pltpu.roll(gy, ny - 1, 0))
            if gx is not None:
                image = image + gx
            if x + 1 < nx:
                after = p_ref[at(j, x + 1), :]
                gx = fx_ref[at(j, x + 1), :] * (after - v)
                image = image - gx
            q_ref[at(j, x), :] = image
            acc = acc + v * image
            if x + 1 < nx:
                v = after
        acc_ref[member(j), :] = acc

    def totals():
        return [jnp.broadcast_to(total(acc_ref[member(j), :]), plane) for j in range(held)]

    def multiply():
        for_members(along_z)
        for_members(apply)
        for j, dot in enumerate(totals()):
            acc_ref[member(j), :] = norm_ref[member(j), :] / dot

    def move(j):
        step = acc_ref[member(j), :]
        for x in range(nx):
            x_ref[at(j, x), :] = x_ref[at(j, x), :] + step * p_ref[at(j, x), :]

    def move_and_leave(j):
        step = acc_ref[member(j), :]
        acc = jnp.zeros(plane, jnp.float32)
        for x in range(nx):
            x_ref[at(j, x), :] = x_ref[at(j, x), :] + step * p_ref[at(j, x), :]
            res = r_ref[at(j, x), :] - step * q_ref[at(j, x), :]
            r_ref[at(j, x), :] = res
            acc = acc + res * res
        acc_ref[member(j), :] = acc

    def turn(j):
        ratio = acc_ref[member(j), :]
        for x in range(nx):
            p_ref[at(j, x), :] = r_ref[at(j, x), :] + ratio * p_ref[at(j, x), :]

    def one(iteration, carry):
        multiply()
        for_members(move_and_leave)
        for j, norm in enumerate(totals()):
            acc_ref[member(j), :] = norm / norm_ref[member(j), :]
            norm_ref[member(j), :] = norm
        for_members(turn)
        return carry

    x_ref[...] = jnp.zeros(x_ref.shape, jnp.float32)
    lax.fori_loop(0, ITERS - 1, one, 0)
    multiply()
    for_members(move)

    for m in range(n_m):
        for s in range(n_s):
            peer = m * n_s + s
            for o in range(n_obs):
                picked = g_ref[pl.ds(peer * rows + (held + 1) * block + o, 1), :].astype(jnp.int32)[0, 0]
                cell = (s * bx + picked // by) * ny + m * by + picked % by
                for j in range(held):
                    out_ref[pl.ds((peer * held + j) * n_obs + o, 1), :] = x_ref[pl.ds(j * nx * ny + cell, 1), :]


def sums_kernel(pred_ref, values_ref, noise_ref, var_ref, out_ref, *, devices):
    members = pred_ref.shape[0]
    held = members // devices
    pred = pred_ref[...]
    inv_sigma = 1.0 / jnp.sqrt(var_ref[...])
    mean = jnp.sum(pred, axis=0, keepdims=True) / members
    spread = (pred - mean) * inv_sigma
    misfit = (values_ref[...] - pred) * inv_sigma + noise_ref[...]
    by_last = (((1,), (1,)), ((), ()))
    gram = lax.dot_general(spread, spread, by_last, precision=HIGHEST, preferred_element_type=jnp.float32)
    cross = lax.dot_general(spread, misfit, by_last, precision=HIGHEST, preferred_element_type=jnp.float32)
    for d in range(devices):
        out_ref[d, 0:held, :] = gram[d * held : (d + 1) * held, :]
        out_ref[d, held : 2 * held, :] = cross[d * held : (d + 1) * held, :]


def update_kernel(sums_ref, field_ref, out_ref, a_ref, c_ref, *, devices):
    members = sums_ref.shape[2]
    held = members // devices
    tile = 8
    for d in range(devices):
        a_ref[pl.ds(d * held, held), :] = sums_ref[d, 0:held, :]
        c_ref[pl.ds(d * held, held), :] = sums_ref[d, held : 2 * held, :]
    lane = lax.broadcasted_iota(jnp.int32, (tile, members), 1)
    sub = lax.broadcasted_iota(jnp.int32, (tile, members), 0)
    blocks = members // tile
    left, right = [], []
    for k in range(blocks):
        own = (lane == sub + k * tile).astype(jnp.float32) * (members - 1.0)
        left.append(a_ref[pl.ds(k * tile, tile), :] + own)
        right.append(c_ref[pl.ds(k * tile, tile), :])
    wide = (tile, members)

    def row(x, t):
        return jnp.broadcast_to(x[t : t + 1, :], wide)

    def column(x, t):
        return jnp.broadcast_to(x[:, t : t + 1], wide)

    for k in range(blocks):
        parts = [column(left[k], k * tile + t) for t in range(tile)] + [left[k], right[k]]
        for t in range(tile):
            inverse = 1.0 / row(parts[t], t)
            factor = jnp.where(sub == t, 0.0, parts[t] * inverse)
            scaled = sub == t
            for i in range(t + 1, len(parts)):
                pivot = row(parts[i], t)
                parts[i] = jnp.where(scaled, pivot * inverse, parts[i] - factor * pivot)
        left[k], right[k] = parts[-2], parts[-1]
        rows_left = [row(left[k], t) for t in range(tile)]
        rows_right = [row(right[k], t) for t in range(tile)]
        for i in range(blocks):
            if i != k:
                columns = [column(left[i], k * tile + t) for t in range(tile)]
                for t in range(tile):
                    right[i] = right[i] - columns[t] * rows_right[t]
                    if k + 1 < blocks:
                        left[i] = left[i] - columns[t] * rows_left[t]
    for k in range(blocks):
        c_ref[pl.ds(k * tile, tile), :] = right[k]
    weights = c_ref[...]
    cells = field_ref.shape[0] // members
    by_first = (((0,), (0,)), ((), ()))
    for c in range(cells):
        field = field_ref[pl.ds(c, members, stride=cells), :]
        anomaly = field - jnp.sum(field, axis=0, keepdims=True) / members
        moved = lax.dot_general(weights, anomaly, by_first, precision=HIGHEST, preferred_element_type=jnp.float32)
        out_ref[pl.ds(c, members, stride=cells), :] = field + moved


def exchange(x):
    return lax.all_to_all(x, AXES, split_axis=0, concat_axis=0, tiled=True)


def local_whole(ensemble, source, obs_rows, obs_values, obs_noise, obs_var):
    members = ensemble.shape[0]
    bx, by, nz = source.shape
    n_m, n_s = lax.axis_size("member"), lax.axis_size("space")
    devices = n_m * n_s
    held = members // devices
    block = bx * by
    n_obs = obs_rows.shape[-1]
    wide = (devices, block, 1, nz)
    packed = jnp.concatenate(
        [
            ensemble.reshape(devices, held * block, 1, nz),
            jnp.broadcast_to(source.reshape(1, block, 1, nz), wide),
            jnp.broadcast_to(obs_rows.astype(jnp.float32).reshape(1, n_obs, 1, 1), (devices, n_obs, 1, nz)),
        ],
        axis=1,
    )
    rows = packed.shape[1]
    got = exchange(packed.reshape(devices * rows, 1, nz)).reshape(devices * rows, nz)
    nx, ny = n_s * bx, n_m * by
    field = (held * nx * ny, nz)
    picked = vmem_call(
        functools.partial(pressure_kernel, dims=(n_m, n_s, held, bx, by, n_obs)),
        (members * n_obs, nz),
        [field] * 9 + [(held * ny, nz)] * 2,
        "pressure",
        got,
    )
    returned = exchange(picked.reshape(members * n_obs, 1, nz))
    sums = vmem_call(
        functools.partial(sums_kernel, devices=devices),
        (devices, 2 * held, members),
        [],
        "sums",
        returned.reshape(members, n_obs * nz),
        obs_values.reshape(1, -1),
        obs_noise.reshape(members, -1),
        obs_var.reshape(1, -1),
    )
    own = jnp.sum(exchange(sums), axis=0, keepdims=True)
    gathered = exchange(jnp.broadcast_to(own, sums.shape))
    updated = vmem_call(
        functools.partial(update_kernel, devices=devices),
        (members * block, nz),
        [(members, members)] * 2,
        "update",
        gathered,
        ensemble.reshape(members * block, nz),
    )
    return (updated.reshape(ensemble.shape), returned.reshape(members, 1, 1, n_obs * nz))


def local(ensemble, *rest):
    devices = lax.axis_size("member") * lax.axis_size("space")
    form = local_whole if ensemble.shape[0] % devices == 0 else local_split
    return form(ensemble, *rest)


def solution(mesh):
    in_specs = (
        P(None, "space", "member", None),
        P("space", "member", None),
        P("space", "member", None),
        P("space", "member", None),
        P(None, "space", "member", None),
        P("space", "member", None),
    )
    out_specs = (P(None, "space", "member", None), P(None, "space", "member", None))
    return jax.shard_map(local, mesh=mesh, in_specs=in_specs, out_specs=out_specs, check_vma=False)
```

```python
import functools

import jax
import jax.numpy as jnp
from jax import lax
from jax.experimental import pallas as pl
from jax.experimental.pallas import tpu as pltpu
from jax.sharding import PartitionSpec as P

ITERS = 4
AXES = ("member", "space")
HIGHEST = lax.Precision.HIGHEST


def padded_2(x, sides, width):
    for axis, dim in sides:
        devices, length = (lax.axis_size(axis), x.shape[dim])
        up = [(i, (i + 1) % devices) for i in range(devices - 1)]
        down = [(j, i) for i, j in up]
        last = lax.slice_in_dim(x, length - width, length, axis=dim)
        leading = lax.slice_in_dim(x, 0, width, axis=dim)
        before = lax.ppermute(last, axis, up)
        after = lax.ppermute(leading, axis, down)
        x = jnp.concatenate([before, x, after], axis=dim)
    return x


def harmonic(first_cond, second_cond):
    return 2.0 * first_cond * second_cond / (first_cond + second_cond)


def extend(values_in):
    widened = padded_2(values_in, (("member", 2),), 1)
    return jnp.pad(widened, ((0, 0), (1, 1), (0, 0), (1, 1)))


def member_dots(dot_terms):
    return lax.psum(dot_terms, "member")


def face_terms(cond):
    widened = extend(cond)
    edge_pad = jnp.pad(cond, ((0, 0), (1, 1), (1, 1), (1, 1)), mode="edge")
    cond_pad = jnp.where(widened > 0.0, widened, edge_pad)
    face_x = harmonic(cond_pad[:, :-1, 1:-1, 1:-1], cond_pad[:, 1:, 1:-1, 1:-1])
    face_y = harmonic(cond_pad[:, 1:-1, :-1, 1:-1], cond_pad[:, 1:-1, 1:, 1:-1])
    face_z = harmonic(cond, cond_pad[:, 1:-1, 1:-1, 2:])
    lower_z = jnp.concatenate([harmonic(cond[..., :1], cond[..., :1]), face_z[..., :-1]], axis=-1)
    return (face_x, face_y, face_z, lower_z)


def operate(values_in, face_x, face_y, face_z, lower_z):
    padded = extend(values_in)
    result = face_x[:, 1:] * (values_in - padded[:, 2:, 1:-1, 1:-1]) + face_x[:, :-1] * (
        values_in - padded[:, :-2, 1:-1, 1:-1]
    )
    result = (
        result
        + face_y[:, :, 1:] * (values_in - padded[:, 1:-1, 2:, 1:-1])
        + face_y[:, :, :-1] * (values_in - padded[:, 1:-1, :-2, 1:-1])
    )
    result = (
        result
        + face_z * (values_in - padded[:, 1:-1, 1:-1, 2:])
        + lower_z * (values_in - padded[:, 1:-1, 1:-1, :-2])
    )
    return result


def conjugate(cond, forcing):
    face_x, face_y, face_z, lower_z = face_terms(cond)
    residual = jnp.broadcast_to(forcing[None], cond.shape)
    direction = residual
    solution = jnp.zeros_like(cond)
    norm_now = member_dots(jnp.sum(residual * residual, axis=(1, 2, 3)))
    for iteration in range(ITERS):
        image = operate(direction, face_x, face_y, face_z, lower_z)
        step_size = norm_now / member_dots(jnp.sum(direction * image, axis=(1, 2, 3)))
        solution = solution + step_size[:, None, None, None] * direction
        residual = residual - step_size[:, None, None, None] * image
        if iteration + 1 < ITERS:
            norm_next = member_dots(jnp.sum(residual * residual, axis=(1, 2, 3)))
            direction = residual + (norm_next / norm_now)[:, None, None, None] * direction
            norm_now = norm_next
    return solution


def local_split(ensemble, source, obs_rows, obs_values, obs_noise, obs_var):
    total_members = ensemble.shape[0]
    block_x, block_y, layers = source.shape
    held_fields = lax.all_to_all(ensemble, "space", split_axis=0, concat_axis=1, tiled=True)
    forcing = lax.all_gather(source, "space", axis=0, tiled=True)
    pressure = conjugate(jnp.exp(held_fields), forcing)
    held_count = pressure.shape[0]
    cells_flat = pressure.reshape(held_count, -1, layers)
    gathered_rows = lax.all_gather(obs_rows, "space", axis=0, tiled=True)
    row_ids = gathered_rows[:, 0]
    peer_ids = jnp.arange(row_ids.shape[0], dtype=jnp.int32)[:, None]
    flat_index = (peer_ids * block_x + row_ids // block_y) * block_y + row_ids % block_y
    picked = jnp.take(cells_flat, flat_index.reshape(-1), axis=1)
    returned = lax.all_to_all(picked, "space", split_axis=1, concat_axis=0, tiled=True)
    predicted = returned.reshape(total_members, 1, 1, -1)
    flat_pred = returned.reshape(total_members, -1)
    inv_sigma = 1.0 / jnp.sqrt(obs_var.reshape(-1))
    spread = (flat_pred - jnp.mean(flat_pred, axis=0)) * inv_sigma
    misfit = (obs_values.reshape(-1) - flat_pred) * inv_sigma + obs_noise.reshape(total_members, -1)
    gram_part = jnp.dot(spread, spread.T, precision=HIGHEST)
    cross_part = jnp.dot(spread, misfit.T, precision=HIGHEST)
    gram_sum, cross_sum = lax.psum((gram_part, cross_part), AXES)
    factor = jnp.linalg.cholesky(
        gram_sum + (total_members - 1.0) * jnp.eye(total_members, dtype=jnp.float32)
    )
    weights = jax.scipy.linalg.cho_solve((factor, True), cross_sum)
    flat_field = ensemble.reshape(total_members, -1)
    anomalies = flat_field - jnp.mean(flat_field, axis=0)
    updated = flat_field + jnp.dot(weights.T, anomalies, precision=HIGHEST)
    return (updated.reshape(ensemble.shape), predicted)


def vmem_call(kernel, out, scratch, name, *operands, spaces=None):
    specs = [pl.BlockSpec(memory_space=s) for s in spaces or [pltpu.VMEM] * len(operands)]
    return pl.pallas_call(
        kernel,
        out_shape=out,
        in_specs=specs,
        out_specs=pl.BlockSpec(memory_space=pltpu.VMEM),
        scratch_shapes=scratch,
        name=name,
    )(*operands)


def near(x):
    return pltpu.with_memory_space_constraint(x, pltpu.VMEM)


def pack_kernel(field_ref, source_ref, obs_ref, out_ref, sems):
    devices, rows, _, nz = out_ref.shape
    cells, block, n_obs = field_ref.shape[1], source_ref.shape[0], obs_ref.shape[0]
    copies = [
        pltpu.make_async_copy(field_ref.at[d], out_ref.at[d, pl.ds(0, cells)], sems.at[d]) for d in range(devices)
    ]
    for copy in copies:
        copy.start()
    source = source_ref[...]
    picks = [jnp.full((1, 1, nz), obs_ref[o].astype(jnp.float32)) for o in range(n_obs)]
    for d in range(devices):
        out_ref[d, pl.ds(cells, block)] = source
        for o in range(n_obs):
            out_ref[d, pl.ds(cells + block + o, 1)] = picks[o]
    for copy in copies:
        copy.wait()


def total(acc):
    return jnp.sum(jnp.sum(acc, axis=0, keepdims=True), axis=1, keepdims=True)


def pressure_kernel(g_ref, out_ref, e_ref, fx_ref, fy_ref, fz_ref, bd_ref, p_ref, r_ref, q_ref, x_ref, acc_ref, norm_ref, *, dims):
    n_m, n_s, held, bx, by, n_obs = dims
    nx, ny = n_s * bx, n_m * by
    nz = g_ref.shape[1]
    block = bx * by
    rows = (held + 1) * block + n_obs
    plane = (ny, nz)
    lane = lax.broadcasted_iota(jnp.int32, plane, 1)
    sub = lax.broadcasted_iota(jnp.int32, plane, 0)

    def at(j, x):
        return pl.ds(pl.multiple_of((j * nx + x) * ny, ny), ny)

    def member(j):
        return pl.ds(pl.multiple_of(j * ny, ny), ny)

    def for_members(fn):
        def body(j, carry):
            fn(j)
            return carry

        lax.fori_loop(0, held, body, 0)

    for m in range(n_m):
        for s in range(n_s):
            base = (m * n_s + s) * rows
            for a in range(bx):
                x = s * bx + a
                for j in range(held):
                    e_ref[pl.ds((j * nx + x) * ny + m * by, by), :] = g_ref[
                        pl.ds(base + j * block + a * by, by), :
                    ]
                x_ref[pl.ds(x * ny + m * by, by), :] = g_ref[pl.ds(base + held * block + a * by, by), :]

    edge_z = (lane == 0).astype(jnp.float32) + (lane == nz - 1).astype(jnp.float32)
    edge_y = (sub == 0).astype(jnp.float32) + (sub == ny - 1).astype(jnp.float32)
    norm0 = jnp.zeros(plane, jnp.float32)
    for x in range(nx):
        v = x_ref[at(0, x), :]
        norm0 = norm0 + v * v
        for j in range(held):
            p_ref[at(j, x), :] = v
            r_ref[at(j, x), :] = v
    norm0 = jnp.broadcast_to(total(norm0), plane)
    for j in range(held):
        norm_ref[member(j), :] = norm0

    def faces(j):
        before = None
        for x in range(nx):
            e = jnp.exp(-e_ref[at(j, x), :])
            if before is not None:
                fx_ref[at(j, x), :] = 2.0 / (e + before)
            fy_ref[at(j, x), :] = jnp.where(sub > 0, 2.0 / (e + pltpu.roll(e, 1, 0)), 0.0)
            fz_ref[at(j, x), :] = jnp.where(lane > 0, 2.0 / (e + pltpu.roll(e, 1, 1)), 0.0)
            ends = edge_y + edge_z
            if x == 0 or x == nx - 1:
                ends = ends + 1.0
            bd_ref[at(j, x), :] = ends / e
            before = e

    for_members(faces)

    def along_z(j):
        for x in range(nx):
            v = p_ref[at(j, x), :]
            gz = fz_ref[at(j, x), :] * (v - pltpu.roll(v, 1, 1))
            q_ref[at(j, x), :] = gz - pltpu.roll(gz, nz - 1, 1)

    def apply(j):
        acc = jnp.zeros(plane, jnp.float32)
        v = p_ref[at(j, 0), :]
        gx = None
        for x in range(nx):
            gy = fy_ref[at(j, x), :] * (v - pltpu.roll(v, 1, 0))
            image = q_ref[at(j, x), :] + bd_ref[at(j, x), :] * v
            image = image + (gy - pltpu.roll(gy, ny - 1, 0))
            if gx is not None:
                image = image + gx
            if x + 1 < nx:
                after = p_ref[at(j, x + 1), :]
                gx = fx_ref[at(j, x + 1), :] * (after - v)
                image = image - gx
            q_ref[at(j, x), :] = image
            acc = acc + v * image
            if x + 1 < nx:
                v = after
        acc_ref[member(j), :] = acc

    def totals():
        return [jnp.broadcast_to(total(acc_ref[member(j), :]), plane) for j in range(held)]

    def multiply():
        for_members(along_z)
        for_members(apply)
        for j, dot in enumerate(totals()):
            acc_ref[member(j), :] = norm_ref[member(j), :] / dot

    def move(j):
        step = acc_ref[member(j), :]
        for x in range(nx):
            x_ref[at(j, x), :] = x_ref[at(j, x), :] + step * p_ref[at(j, x), :]

    def move_and_leave(j):
        step = acc_ref[member(j), :]
        acc = jnp.zeros(plane, jnp.float32)
        for x in range(nx):
            x_ref[at(j, x), :] = x_ref[at(j, x), :] + step * p_ref[at(j, x), :]
            res = r_ref[at(j, x), :] - step * q_ref[at(j, x), :]
            r_ref[at(j, x), :] = res
            acc = acc + res * res
        acc_ref[member(j), :] = acc

    def turn(j):
        ratio = acc_ref[member(j), :]
        for x in range(nx):
            p_ref[at(j, x), :] = r_ref[at(j, x), :] + ratio * p_ref[at(j, x), :]

    def one(iteration, carry):
        multiply()
        for_members(move_and_leave)
        for j, norm in enumerate(totals()):
            acc_ref[member(j), :] = norm / norm_ref[member(j), :]
            norm_ref[member(j), :] = norm
        for_members(turn)
        return carry

    x_ref[...] = jnp.zeros(x_ref.shape, jnp.float32)
    lax.fori_loop(0, ITERS - 1, one, 0)
    multiply()
    for_members(move)

    for m in range(n_m):
        for s in range(n_s):
            peer = m * n_s + s
            for o in range(n_obs):
                picked = g_ref[pl.ds(peer * rows + (held + 1) * block + o, 1), :].astype(jnp.int32)[0, 0]
                cell = (s * bx + picked // by) * ny + m * by + picked % by
                for j in range(held):
                    out_ref[pl.ds((peer * held + j) * n_obs + o, 1), :] = x_ref[pl.ds(j * nx * ny + cell, 1), :]


def sums_kernel(pred_ref, values_ref, noise_ref, var_ref, out_ref, *, devices):
    members = pred_ref.shape[0]
    held = members // devices
    pred = pred_ref[...]
    inv_sigma = 1.0 / jnp.sqrt(var_ref[...])
    mean = jnp.sum(pred, axis=0, keepdims=True) / members
    spread = (pred - mean) * inv_sigma
    misfit = (values_ref[...] - pred) * inv_sigma + noise_ref[...]
    by_last = (((1,), (1,)), ((), ()))
    gram = lax.dot_general(spread, spread, by_last, precision=HIGHEST, preferred_element_type=jnp.float32)
    cross = lax.dot_general(spread, misfit, by_last, precision=HIGHEST, preferred_element_type=jnp.float32)
    for d in range(devices):
        out_ref[d, 0:held, :] = gram[d * held : (d + 1) * held, :]
        out_ref[d, held : 2 * held, :] = cross[d * held : (d + 1) * held, :]


def update_kernel(sums_ref, field_ref, out_ref, a_ref, c_ref, *, devices):
    members = sums_ref.shape[2]
    held = members // devices
    tile = 8
    for d in range(devices):
        a_ref[pl.ds(d * held, held), :] = sums_ref[d, 0:held, :]
        c_ref[pl.ds(d * held, held), :] = sums_ref[d, held : 2 * held, :]
    lane = lax.broadcasted_iota(jnp.int32, (tile, members), 1)
    sub = lax.broadcasted_iota(jnp.int32, (tile, members), 0)
    blocks = members // tile
    left, right = [], []
    for k in range(blocks):
        own = (lane == sub + k * tile).astype(jnp.float32) * (members - 1.0)
        left.append(a_ref[pl.ds(k * tile, tile), :] + own)
        right.append(c_ref[pl.ds(k * tile, tile), :])
    wide = (tile, members)

    def row(x, t):
        return jnp.broadcast_to(x[t : t + 1, :], wide)

    def column(x, t):
        return jnp.broadcast_to(x[:, t : t + 1], wide)

    for k in range(blocks):
        parts = [column(left[k], k * tile + t) for t in range(tile)] + [left[k], right[k]]
        for t in range(tile):
            inverse = 1.0 / row(parts[t], t)
            factor = jnp.where(sub == t, 0.0, parts[t] * inverse)
            scaled = sub == t
            for i in range(t + 1, len(parts)):
                pivot = row(parts[i], t)
                parts[i] = jnp.where(scaled, pivot * inverse, parts[i] - factor * pivot)
        left[k], right[k] = parts[-2], parts[-1]
        rows_left = [row(left[k], t) for t in range(tile)]
        rows_right = [row(right[k], t) for t in range(tile)]
        for i in range(blocks):
            if i != k:
                columns = [column(left[i], k * tile + t) for t in range(tile)]
                for t in range(tile):
                    right[i] = right[i] - columns[t] * rows_right[t]
                    if k + 1 < blocks:
                        left[i] = left[i] - columns[t] * rows_left[t]
    for k in range(blocks):
        c_ref[pl.ds(k * tile, tile), :] = right[k]
    weights = c_ref[...]
    cells = field_ref.shape[0] // members
    by_first = (((0,), (0,)), ((), ()))
    for c in range(cells):
        field = field_ref[pl.ds(c, members, stride=cells), :]
        anomaly = field - jnp.sum(field, axis=0, keepdims=True) / members
        moved = lax.dot_general(weights, anomaly, by_first, precision=HIGHEST, preferred_element_type=jnp.float32)
        out_ref[pl.ds(c, members, stride=cells), :] = field + moved


def exchange(x):
    return lax.all_to_all(x, AXES, split_axis=0, concat_axis=0, tiled=True)


def local_whole(ensemble, source, obs_rows, obs_values, obs_noise, obs_var):
    members = ensemble.shape[0]
    bx, by, nz = source.shape
    n_m, n_s = lax.axis_size("member"), lax.axis_size("space")
    devices = n_m * n_s
    held = members // devices
    block = bx * by
    n_obs = obs_rows.shape[-1]
    rows = (held + 1) * block + n_obs
    packed = vmem_call(
        pack_kernel,
        pltpu.VMEM((devices, rows, 1, nz), jnp.float32),
        [pltpu.SemaphoreType.DMA((devices,))],
        "pack",
        ensemble.reshape(devices, held * block, 1, nz),
        source.reshape(block, 1, nz),
        obs_rows.reshape(-1),
        spaces=[pl.ANY, pltpu.VMEM, pltpu.SMEM],
    )
    got = exchange(packed.reshape(devices * rows, 1, nz)).reshape(devices * rows, nz)
    nx, ny = n_s * bx, n_m * by
    field = pltpu.VMEM((held * nx * ny, nz), jnp.float32)
    plane = pltpu.VMEM((held * ny, nz), jnp.float32)
    picked = vmem_call(
        functools.partial(pressure_kernel, dims=(n_m, n_s, held, bx, by, n_obs)),
        pltpu.VMEM((members * n_obs, nz), jnp.float32),
        [field] * 9 + [plane] * 2,
        "pressure",
        near(got),
    )
    returned = exchange(picked.reshape(members * n_obs, 1, nz))
    sums = vmem_call(
        functools.partial(sums_kernel, devices=devices),
        pltpu.VMEM((devices, 2 * held, members), jnp.float32),
        [],
        "sums",
        near(returned.reshape(members, n_obs * nz)),
        obs_values.reshape(1, -1),
        near(obs_noise.reshape(members, -1)),
        obs_var.reshape(1, -1),
    )
    own = jnp.sum(exchange(sums), axis=0, keepdims=True)
    gathered = exchange(jnp.broadcast_to(own, sums.shape))
    updated = vmem_call(
        functools.partial(update_kernel, devices=devices),
        jax.ShapeDtypeStruct((members * block, nz), jnp.float32),
        [pltpu.VMEM((members, members), jnp.float32)] * 2,
        "update",
        near(gathered),
        near(ensemble.reshape(members * block, nz)),
    )
    return (updated.reshape(ensemble.shape), returned.reshape(members, 1, 1, n_obs * nz))


def local(ensemble, *rest):
    devices = lax.axis_size("member") * lax.axis_size("space")
    form = local_whole if ensemble.shape[0] % devices == 0 else local_split
    return form(ensemble, *rest)


def solution(mesh):
    in_specs = (
        P(None, "space", "member", None),
        P("space", "member", None),
        P("space", "member", None),
        P("space", "member", None),
        P(None, "space", "member", None),
        P("space", "member", None),
    )
    out_specs = (P(None, "space", "member", None), P(None, "space", "member", None))
    return jax.shard_map(local, mesh=mesh, in_specs=in_specs, out_specs=out_specs, check_vma=False)
```

```python
import functools

import jax
import jax.numpy as jnp
from jax import lax
from jax.experimental import pallas as pl
from jax.experimental.pallas import tpu as pltpu
from jax.sharding import PartitionSpec as P

ITERS = 4
AXES = ("member", "space")
HIGHEST = lax.Precision.HIGHEST


def padded_2(x, sides, width):
    for axis, dim in sides:
        devices, length = (lax.axis_size(axis), x.shape[dim])
        up = [(i, (i + 1) % devices) for i in range(devices - 1)]
        down = [(j, i) for i, j in up]
        last = lax.slice_in_dim(x, length - width, length, axis=dim)
        leading = lax.slice_in_dim(x, 0, width, axis=dim)
        before = lax.ppermute(last, axis, up)
        after = lax.ppermute(leading, axis, down)
        x = jnp.concatenate([before, x, after], axis=dim)
    return x


def harmonic(first_cond, second_cond):
    return 2.0 * first_cond * second_cond / (first_cond + second_cond)


def extend(values_in):
    widened = padded_2(values_in, (("member", 2),), 1)
    return jnp.pad(widened, ((0, 0), (1, 1), (0, 0), (1, 1)))


def member_dots(dot_terms):
    return lax.psum(dot_terms, "member")


def face_terms(cond):
    widened = extend(cond)
    edge_pad = jnp.pad(cond, ((0, 0), (1, 1), (1, 1), (1, 1)), mode="edge")
    cond_pad = jnp.where(widened > 0.0, widened, edge_pad)
    face_x = harmonic(cond_pad[:, :-1, 1:-1, 1:-1], cond_pad[:, 1:, 1:-1, 1:-1])
    face_y = harmonic(cond_pad[:, 1:-1, :-1, 1:-1], cond_pad[:, 1:-1, 1:, 1:-1])
    face_z = harmonic(cond, cond_pad[:, 1:-1, 1:-1, 2:])
    lower_z = jnp.concatenate([harmonic(cond[..., :1], cond[..., :1]), face_z[..., :-1]], axis=-1)
    return (face_x, face_y, face_z, lower_z)


def operate(values_in, face_x, face_y, face_z, lower_z):
    padded = extend(values_in)
    result = face_x[:, 1:] * (values_in - padded[:, 2:, 1:-1, 1:-1]) + face_x[:, :-1] * (
        values_in - padded[:, :-2, 1:-1, 1:-1]
    )
    result = (
        result
        + face_y[:, :, 1:] * (values_in - padded[:, 1:-1, 2:, 1:-1])
        + face_y[:, :, :-1] * (values_in - padded[:, 1:-1, :-2, 1:-1])
    )
    result = (
        result
        + face_z * (values_in - padded[:, 1:-1, 1:-1, 2:])
        + lower_z * (values_in - padded[:, 1:-1, 1:-1, :-2])
    )
    return result


def conjugate(cond, forcing):
    face_x, face_y, face_z, lower_z = face_terms(cond)
    residual = jnp.broadcast_to(forcing[None], cond.shape)
    direction = residual
    solution = jnp.zeros_like(cond)
    norm_now = member_dots(jnp.sum(residual * residual, axis=(1, 2, 3)))
    for iteration in range(ITERS):
        image = operate(direction, face_x, face_y, face_z, lower_z)
        step_size = norm_now / member_dots(jnp.sum(direction * image, axis=(1, 2, 3)))
        solution = solution + step_size[:, None, None, None] * direction
        residual = residual - step_size[:, None, None, None] * image
        if iteration + 1 < ITERS:
            norm_next = member_dots(jnp.sum(residual * residual, axis=(1, 2, 3)))
            direction = residual + (norm_next / norm_now)[:, None, None, None] * direction
            norm_now = norm_next
    return solution


def local_split(ensemble, source, obs_rows, obs_values, obs_noise, obs_var):
    total_members = ensemble.shape[0]
    block_x, block_y, layers = source.shape
    held_fields = lax.all_to_all(ensemble, "space", split_axis=0, concat_axis=1, tiled=True)
    forcing = lax.all_gather(source, "space", axis=0, tiled=True)
    pressure = conjugate(jnp.exp(held_fields), forcing)
    held_count = pressure.shape[0]
    cells_flat = pressure.reshape(held_count, -1, layers)
    gathered_rows = lax.all_gather(obs_rows, "space", axis=0, tiled=True)
    row_ids = gathered_rows[:, 0]
    peer_ids = jnp.arange(row_ids.shape[0], dtype=jnp.int32)[:, None]
    flat_index = (peer_ids * block_x + row_ids // block_y) * block_y + row_ids % block_y
    picked = jnp.take(cells_flat, flat_index.reshape(-1), axis=1)
    returned = lax.all_to_all(picked, "space", split_axis=1, concat_axis=0, tiled=True)
    predicted = returned.reshape(total_members, 1, 1, -1)
    flat_pred = returned.reshape(total_members, -1)
    inv_sigma = 1.0 / jnp.sqrt(obs_var.reshape(-1))
    spread = (flat_pred - jnp.mean(flat_pred, axis=0)) * inv_sigma
    misfit = (obs_values.reshape(-1) - flat_pred) * inv_sigma + obs_noise.reshape(total_members, -1)
    gram_part = jnp.dot(spread, spread.T, precision=HIGHEST)
    cross_part = jnp.dot(spread, misfit.T, precision=HIGHEST)
    gram_sum, cross_sum = lax.psum((gram_part, cross_part), AXES)
    factor = jnp.linalg.cholesky(
        gram_sum + (total_members - 1.0) * jnp.eye(total_members, dtype=jnp.float32)
    )
    weights = jax.scipy.linalg.cho_solve((factor, True), cross_sum)
    flat_field = ensemble.reshape(total_members, -1)
    anomalies = flat_field - jnp.mean(flat_field, axis=0)
    updated = flat_field + jnp.dot(weights.T, anomalies, precision=HIGHEST)
    return (updated.reshape(ensemble.shape), predicted)


def vmem_call(kernel, out, scratch, name, *operands, spaces=None, outs=pl.BlockSpec(memory_space=pltpu.VMEM)):
    specs = [pl.BlockSpec(memory_space=s) for s in spaces or [pltpu.VMEM] * len(operands)]
    return pl.pallas_call(
        kernel,
        out_shape=out,
        in_specs=specs,
        out_specs=outs,
        scratch_shapes=scratch,
        name=name,
    )(*operands)


def near(x):
    return pltpu.with_memory_space_constraint(x, pltpu.VMEM)


def pack_kernel(field_ref, source_ref, obs_ref, out_ref, block_ref, rows_ref, sems):
    devices, _, _, nz = out_ref.shape
    cells, block, n_obs = field_ref.shape[1], source_ref.shape[0], obs_ref.shape[0]
    fields = pltpu.make_async_copy(field_ref, out_ref.at[:, pl.ds(0, cells)], sems.at[0])
    source = pltpu.make_async_copy(source_ref, block_ref, sems.at[1])
    rows = pltpu.make_async_copy(obs_ref, rows_ref, sems.at[2])
    rows.start()
    source.start()
    fields.start()
    rows.wait()
    for o in range(n_obs):
        pick = jnp.full((1, 1, nz), rows_ref[o].astype(jnp.float32))
        for d in range(devices):
            out_ref[d, pl.ds(cells + block + o, 1)] = pick
    source.wait()
    held = block_ref[...]
    for d in range(devices):
        out_ref[d, pl.ds(cells, block)] = held
    fields.wait()


def total(acc):
    return jnp.sum(jnp.sum(acc, axis=0, keepdims=True), axis=1, keepdims=True)


def pressure_kernel(g_ref, out_ref, e_ref, fx_ref, fy_ref, fz_ref, bd_ref, p_ref, r_ref, q_ref, x_ref, acc_ref, norm_ref, *, dims):
    n_m, n_s, held, bx, by, n_obs = dims
    nx, ny = n_s * bx, n_m * by
    nz = g_ref.shape[1]
    block = bx * by
    rows = (held + 1) * block + n_obs
    plane = (ny, nz)
    lane = lax.broadcasted_iota(jnp.int32, plane, 1)
    sub = lax.broadcasted_iota(jnp.int32, plane, 0)

    def at(j, x):
        return pl.ds(pl.multiple_of((j * nx + x) * ny, ny), ny)

    def member(j):
        return pl.ds(pl.multiple_of(j * ny, ny), ny)

    def for_members(fn):
        def body(j, carry):
            fn(j)
            return carry

        lax.fori_loop(0, held, body, 0)

    for m in range(n_m):
        for s in range(n_s):
            base = (m * n_s + s) * rows
            for a in range(bx):
                x = s * bx + a
                for j in range(held):
                    e_ref[pl.ds((j * nx + x) * ny + m * by, by), :] = g_ref[
                        pl.ds(base + j * block + a * by, by), :
                    ]
                x_ref[pl.ds(x * ny + m * by, by), :] = g_ref[pl.ds(base + held * block + a * by, by), :]

    edge_z = (lane == 0).astype(jnp.float32) + (lane == nz - 1).astype(jnp.float32)
    edge_y = (sub == 0).astype(jnp.float32) + (sub == ny - 1).astype(jnp.float32)
    norm0 = jnp.zeros(plane, jnp.float32)
    for x in range(nx):
        v = x_ref[at(0, x), :]
        norm0 = norm0 + v * v
        for j in range(held):
            p_ref[at(j, x), :] = v
            r_ref[at(j, x), :] = v
    norm0 = jnp.broadcast_to(total(norm0), plane)
    for j in range(held):
        norm_ref[member(j), :] = norm0

    def faces(j):
        before = None
        for x in range(nx):
            e = jnp.exp(-e_ref[at(j, x), :])
            if before is not None:
                fx_ref[at(j, x), :] = 2.0 / (e + before)
            fy_ref[at(j, x), :] = jnp.where(sub > 0, 2.0 / (e + pltpu.roll(e, 1, 0)), 0.0)
            fz_ref[at(j, x), :] = jnp.where(lane > 0, 2.0 / (e + pltpu.roll(e, 1, 1)), 0.0)
            ends = edge_y + edge_z
            if x == 0 or x == nx - 1:
                ends = ends + 1.0
            bd_ref[at(j, x), :] = ends / e
            before = e

    for_members(faces)

    def along_z(j):
        for x in range(nx):
            v = p_ref[at(j, x), :]
            gz = fz_ref[at(j, x), :] * (v - pltpu.roll(v, 1, 1))
            q_ref[at(j, x), :] = gz - pltpu.roll(gz, nz - 1, 1)

    def apply(j):
        acc = jnp.zeros(plane, jnp.float32)
        v = p_ref[at(j, 0), :]
        gx = None
        for x in range(nx):
            gy = fy_ref[at(j, x), :] * (v - pltpu.roll(v, 1, 0))
            image = q_ref[at(j, x), :] + bd_ref[at(j, x), :] * v
            image = image + (gy - pltpu.roll(gy, ny - 1, 0))
            if gx is not None:
                image = image + gx
            if x + 1 < nx:
                after = p_ref[at(j, x + 1), :]
                gx = fx_ref[at(j, x + 1), :] * (after - v)
                image = image - gx
            q_ref[at(j, x), :] = image
            acc = acc + v * image
            if x + 1 < nx:
                v = after
        acc_ref[member(j), :] = acc

    def totals():
        return [jnp.broadcast_to(total(acc_ref[member(j), :]), plane) for j in range(held)]

    def multiply():
        for_members(along_z)
        for_members(apply)
        for j, dot in enumerate(totals()):
            acc_ref[member(j), :] = norm_ref[member(j), :] / dot

    def move(j):
        step = acc_ref[member(j), :]
        for x in range(nx):
            x_ref[at(j, x), :] = x_ref[at(j, x), :] + step * p_ref[at(j, x), :]

    def move_and_leave(j):
        step = acc_ref[member(j), :]
        acc = jnp.zeros(plane, jnp.float32)
        for x in range(nx):
            x_ref[at(j, x), :] = x_ref[at(j, x), :] + step * p_ref[at(j, x), :]
            res = r_ref[at(j, x), :] - step * q_ref[at(j, x), :]
            r_ref[at(j, x), :] = res
            acc = acc + res * res
        acc_ref[member(j), :] = acc

    def turn(j):
        ratio = acc_ref[member(j), :]
        for x in range(nx):
            p_ref[at(j, x), :] = r_ref[at(j, x), :] + ratio * p_ref[at(j, x), :]

    def one(iteration, carry):
        multiply()
        for_members(move_and_leave)
        for j, norm in enumerate(totals()):
            acc_ref[member(j), :] = norm / norm_ref[member(j), :]
            norm_ref[member(j), :] = norm
        for_members(turn)
        return carry

    x_ref[...] = jnp.zeros(x_ref.shape, jnp.float32)
    lax.fori_loop(0, ITERS - 1, one, 0)
    multiply()
    for_members(move)

    for m in range(n_m):
        for s in range(n_s):
            peer = m * n_s + s
            for o in range(n_obs):
                picked = g_ref[pl.ds(peer * rows + (held + 1) * block + o, 1), :].astype(jnp.int32)[0, 0]
                cell = (s * bx + picked // by) * ny + m * by + picked % by
                for j in range(held):
                    out_ref[pl.ds((peer * held + j) * n_obs + o, 1), :] = x_ref[pl.ds(j * nx * ny + cell, 1), :]


def sums_kernel(pred_ref, values_ref, noise_ref, var_ref, out_ref, *, devices):
    members = pred_ref.shape[0]
    held = members // devices
    pred = pred_ref[...]
    inv_sigma = 1.0 / jnp.sqrt(var_ref[...])
    mean = jnp.sum(pred, axis=0, keepdims=True) / members
    spread = (pred - mean) * inv_sigma
    misfit = (values_ref[...] - pred) * inv_sigma + noise_ref[...]
    by_last = (((1,), (1,)), ((), ()))
    gram = lax.dot_general(spread, spread, by_last, precision=HIGHEST, preferred_element_type=jnp.float32)
    cross = lax.dot_general(spread, misfit, by_last, precision=HIGHEST, preferred_element_type=jnp.float32)
    for d in range(devices):
        out_ref[d, 0:held, :] = gram[d * held : (d + 1) * held, :]
        out_ref[d, held : 2 * held, :] = cross[d * held : (d + 1) * held, :]


def spread_kernel(parts_ref, out_ref):
    devices = parts_ref.shape[0]
    own = jnp.sum(parts_ref[...], axis=0)
    for d in range(devices):
        out_ref[d] = own


def update_kernel(sums_ref, field_ref, found_ref, out_ref, predicted_ref, a_ref, c_ref, sem, *, devices):
    predicted = pltpu.make_async_copy(found_ref, predicted_ref, sem)
    predicted.start()
    members = sums_ref.shape[2]
    held = members // devices
    tile = 8
    for d in range(devices):
        a_ref[pl.ds(d * held, held), :] = sums_ref[d, 0:held, :]
        c_ref[pl.ds(d * held, held), :] = sums_ref[d, held : 2 * held, :]
    lane = lax.broadcasted_iota(jnp.int32, (tile, members), 1)
    sub = lax.broadcasted_iota(jnp.int32, (tile, members), 0)
    blocks = members // tile
    left, right = [], []
    for k in range(blocks):
        own = (lane == sub + k * tile).astype(jnp.float32) * (members - 1.0)
        left.append(a_ref[pl.ds(k * tile, tile), :] + own)
        right.append(c_ref[pl.ds(k * tile, tile), :])
    wide = (tile, members)

    def row(x, t):
        return jnp.broadcast_to(x[t : t + 1, :], wide)

    def column(x, t):
        return jnp.broadcast_to(x[:, t : t + 1], wide)

    for k in range(blocks):
        parts = [column(left[k], k * tile + t) for t in range(tile)] + [left[k], right[k]]
        for t in range(tile):
            inverse = 1.0 / row(parts[t], t)
            factor = jnp.where(sub == t, 0.0, parts[t] * inverse)
            scaled = sub == t
            for i in range(t + 1, len(parts)):
                pivot = row(parts[i], t)
                parts[i] = jnp.where(scaled, pivot * inverse, parts[i] - factor * pivot)
        left[k], right[k] = parts[-2], parts[-1]
        rows_left = [row(left[k], t) for t in range(tile)]
        rows_right = [row(right[k], t) for t in range(tile)]
        for i in range(blocks):
            if i != k:
                columns = [column(left[i], k * tile + t) for t in range(tile)]
                for t in range(tile):
                    right[i] = right[i] - columns[t] * rows_right[t]
                    if k + 1 < blocks:
                        left[i] = left[i] - columns[t] * rows_left[t]
    for k in range(blocks):
        c_ref[pl.ds(k * tile, tile), :] = right[k]
    weights = c_ref[...]
    cells = field_ref.shape[0] // members
    by_first = (((0,), (0,)), ((), ()))
    for c in range(cells):
        field = field_ref[pl.ds(c, members, stride=cells), :]
        anomaly = field - jnp.sum(field, axis=0, keepdims=True) / members
        moved = lax.dot_general(weights, anomaly, by_first, precision=HIGHEST, preferred_element_type=jnp.float32)
        out_ref[pl.ds(c, members, stride=cells), :] = field + moved
    predicted.wait()


def exchange(x):
    return lax.all_to_all(x, AXES, split_axis=0, concat_axis=0, tiled=True)


def local_whole(ensemble, source, obs_rows, obs_values, obs_noise, obs_var):
    members = ensemble.shape[0]
    bx, by, nz = source.shape
    n_m, n_s = lax.axis_size("member"), lax.axis_size("space")
    devices = n_m * n_s
    held = members // devices
    block = bx * by
    n_obs = obs_rows.shape[-1]
    rows = (held + 1) * block + n_obs
    packed = vmem_call(
        pack_kernel,
        pltpu.VMEM((devices, rows, 1, nz), jnp.float32),
        [
            pltpu.VMEM((block, 1, nz), jnp.float32),
            pltpu.SMEM((n_obs,), jnp.int32),
            pltpu.SemaphoreType.DMA((3,)),
        ],
        "pack",
        ensemble.reshape(devices, held * block, 1, nz),
        source.reshape(block, 1, nz),
        obs_rows.reshape(-1),
        spaces=[pl.ANY] * 3,
    )
    got = exchange(packed.reshape(devices * rows, 1, nz)).reshape(devices * rows, nz)
    nx, ny = n_s * bx, n_m * by
    field = pltpu.VMEM((held * nx * ny, nz), jnp.float32)
    plane = pltpu.VMEM((held * ny, nz), jnp.float32)
    picked = vmem_call(
        functools.partial(pressure_kernel, dims=(n_m, n_s, held, bx, by, n_obs)),
        pltpu.VMEM((members * n_obs, nz), jnp.float32),
        [field] * 9 + [plane] * 2,
        "pressure",
        near(got),
    )
    returned = exchange(picked.reshape(members * n_obs, 1, nz))
    sums = vmem_call(
        functools.partial(sums_kernel, devices=devices),
        pltpu.VMEM((devices, 2 * held, members), jnp.float32),
        [],
        "sums",
        near(returned.reshape(members, n_obs * nz)),
        obs_values.reshape(1, -1),
        near(obs_noise.reshape(members, -1)),
        obs_var.reshape(1, -1),
    )
    own = vmem_call(spread_kernel, pltpu.VMEM(sums.shape, jnp.float32), [], "spread", near(exchange(sums)))
    gathered = exchange(own)
    updated, predicted = vmem_call(
        functools.partial(update_kernel, devices=devices),
        [
            jax.ShapeDtypeStruct((members * block, nz), jnp.float32),
            jax.ShapeDtypeStruct((members, n_obs * nz), jnp.float32),
        ],
        [pltpu.VMEM((members, members), jnp.float32)] * 2 + [pltpu.SemaphoreType.DMA],
        "update",
        near(gathered),
        near(ensemble.reshape(members * block, nz)),
        near(returned.reshape(members, n_obs * nz)),
        outs=[pl.BlockSpec(memory_space=pltpu.VMEM), pl.BlockSpec(memory_space=pl.ANY)],
    )
    return (updated.reshape(ensemble.shape), predicted.reshape(members, 1, 1, n_obs * nz))


def local(ensemble, *rest):
    devices = lax.axis_size("member") * lax.axis_size("space")
    form = local_whole if ensemble.shape[0] % devices == 0 else local_split
    return form(ensemble, *rest)


def solution(mesh):
    in_specs = (
        P(None, "space", "member", None),
        P("space", "member", None),
        P("space", "member", None),
        P("space", "member", None),
        P(None, "space", "member", None),
        P("space", "member", None),
    )
    out_specs = (P(None, "space", "member", None), P(None, "space", "member", None))
    return jax.shard_map(local, mesh=mesh, in_specs=in_specs, out_specs=out_specs, check_vma=False)
```

```python
import functools

import jax
import jax.numpy as jnp
from jax import lax
from jax.experimental import pallas as pl
from jax.experimental.pallas import tpu as pltpu
from jax.sharding import PartitionSpec as P

ITERS = 4
TILE = 8
UNROLL = 4
AXES = ("member", "space")
HIGHEST = lax.Precision.HIGHEST


def padded_2(x, sides, width):
    for axis, dim in sides:
        devices, length = (lax.axis_size(axis), x.shape[dim])
        up = [(i, (i + 1) % devices) for i in range(devices - 1)]
        down = [(j, i) for i, j in up]
        last = lax.slice_in_dim(x, length - width, length, axis=dim)
        leading = lax.slice_in_dim(x, 0, width, axis=dim)
        before = lax.ppermute(last, axis, up)
        after = lax.ppermute(leading, axis, down)
        x = jnp.concatenate([before, x, after], axis=dim)
    return x


def harmonic(first_cond, second_cond):
    return 2.0 * first_cond * second_cond / (first_cond + second_cond)


def extend(values_in):
    widened = padded_2(values_in, (("member", 2),), 1)
    return jnp.pad(widened, ((0, 0), (1, 1), (0, 0), (1, 1)))


def member_dots(dot_terms):
    return lax.psum(dot_terms, "member")


def face_terms(cond):
    widened = extend(cond)
    edge_pad = jnp.pad(cond, ((0, 0), (1, 1), (1, 1), (1, 1)), mode="edge")
    cond_pad = jnp.where(widened > 0.0, widened, edge_pad)
    face_x = harmonic(cond_pad[:, :-1, 1:-1, 1:-1], cond_pad[:, 1:, 1:-1, 1:-1])
    face_y = harmonic(cond_pad[:, 1:-1, :-1, 1:-1], cond_pad[:, 1:-1, 1:, 1:-1])
    face_z = harmonic(cond, cond_pad[:, 1:-1, 1:-1, 2:])
    lower_z = jnp.concatenate([harmonic(cond[..., :1], cond[..., :1]), face_z[..., :-1]], axis=-1)
    return (face_x, face_y, face_z, lower_z)


def operate(values_in, face_x, face_y, face_z, lower_z):
    padded = extend(values_in)
    result = face_x[:, 1:] * (values_in - padded[:, 2:, 1:-1, 1:-1]) + face_x[:, :-1] * (
        values_in - padded[:, :-2, 1:-1, 1:-1]
    )
    result = (
        result
        + face_y[:, :, 1:] * (values_in - padded[:, 1:-1, 2:, 1:-1])
        + face_y[:, :, :-1] * (values_in - padded[:, 1:-1, :-2, 1:-1])
    )
    result = (
        result
        + face_z * (values_in - padded[:, 1:-1, 1:-1, 2:])
        + lower_z * (values_in - padded[:, 1:-1, 1:-1, :-2])
    )
    return result


def conjugate(cond, forcing):
    face_x, face_y, face_z, lower_z = face_terms(cond)
    residual = jnp.broadcast_to(forcing[None], cond.shape)
    direction = residual
    solution = jnp.zeros_like(cond)
    norm_now = member_dots(jnp.sum(residual * residual, axis=(1, 2, 3)))
    for iteration in range(ITERS):
        image = operate(direction, face_x, face_y, face_z, lower_z)
        step_size = norm_now / member_dots(jnp.sum(direction * image, axis=(1, 2, 3)))
        solution = solution + step_size[:, None, None, None] * direction
        residual = residual - step_size[:, None, None, None] * image
        if iteration + 1 < ITERS:
            norm_next = member_dots(jnp.sum(residual * residual, axis=(1, 2, 3)))
            direction = residual + (norm_next / norm_now)[:, None, None, None] * direction
            norm_now = norm_next
    return solution


def local_split(ensemble, source, obs_rows, obs_values, obs_noise, obs_var):
    total_members = ensemble.shape[0]
    block_x, block_y, layers = source.shape
    held_fields = lax.all_to_all(ensemble, "space", split_axis=0, concat_axis=1, tiled=True)
    forcing = lax.all_gather(source, "space", axis=0, tiled=True)
    pressure = conjugate(jnp.exp(held_fields), forcing)
    held_count = pressure.shape[0]
    cells_flat = pressure.reshape(held_count, -1, layers)
    gathered_rows = lax.all_gather(obs_rows, "space", axis=0, tiled=True)
    row_ids = gathered_rows[:, 0]
    peer_ids = jnp.arange(row_ids.shape[0], dtype=jnp.int32)[:, None]
    flat_index = (peer_ids * block_x + row_ids // block_y) * block_y + row_ids % block_y
    picked = jnp.take(cells_flat, flat_index.reshape(-1), axis=1)
    returned = lax.all_to_all(picked, "space", split_axis=1, concat_axis=0, tiled=True)
    predicted = returned.reshape(total_members, 1, 1, -1)
    flat_pred = returned.reshape(total_members, -1)
    inv_sigma = 1.0 / jnp.sqrt(obs_var.reshape(-1))
    spread = (flat_pred - jnp.mean(flat_pred, axis=0)) * inv_sigma
    misfit = (obs_values.reshape(-1) - flat_pred) * inv_sigma + obs_noise.reshape(total_members, -1)
    gram_part = jnp.dot(spread, spread.T, precision=HIGHEST)
    cross_part = jnp.dot(spread, misfit.T, precision=HIGHEST)
    gram_sum, cross_sum = lax.psum((gram_part, cross_part), AXES)
    factor = jnp.linalg.cholesky(
        gram_sum + (total_members - 1.0) * jnp.eye(total_members, dtype=jnp.float32)
    )
    weights = jax.scipy.linalg.cho_solve((factor, True), cross_sum)
    flat_field = ensemble.reshape(total_members, -1)
    anomalies = flat_field - jnp.mean(flat_field, axis=0)
    updated = flat_field + jnp.dot(weights.T, anomalies, precision=HIGHEST)
    return (updated.reshape(ensemble.shape), predicted)


def vmem_call(kernel, out, scratch, name, *operands, spaces=None, outs=pl.BlockSpec(memory_space=pltpu.VMEM)):
    specs = [pl.BlockSpec(memory_space=s) for s in spaces or [pltpu.VMEM] * len(operands)]
    return pl.pallas_call(
        kernel,
        out_shape=out,
        in_specs=specs,
        out_specs=outs,
        scratch_shapes=scratch,
        name=name,
    )(*operands)


def near(x):
    return pltpu.with_memory_space_constraint(x, pltpu.VMEM)


def pack_kernel(field_ref, source_ref, obs_ref, out_ref, block_ref, rows_ref, sems):
    devices, _, _, nz = out_ref.shape
    cells, block, n_obs = field_ref.shape[1], source_ref.shape[0], obs_ref.shape[0]
    fields = pltpu.make_async_copy(field_ref, out_ref.at[:, pl.ds(0, cells)], sems.at[0])
    source = pltpu.make_async_copy(source_ref, block_ref, sems.at[1])
    rows = pltpu.make_async_copy(obs_ref, rows_ref, sems.at[2])
    rows.start()
    source.start()
    fields.start()
    rows.wait()
    for o in range(n_obs):
        pick = jnp.full((1, 1, nz), rows_ref[o].astype(jnp.float32))
        for d in range(devices):
            out_ref[d, pl.ds(cells + block + o, 1)] = pick
    source.wait()
    held = block_ref[...]
    for d in range(devices):
        out_ref[d, pl.ds(cells, block)] = held
    fields.wait()


def total(acc):
    return jnp.sum(jnp.sum(acc, axis=0, keepdims=True), axis=1, keepdims=True)


def pressure_kernel(g_ref, out_ref, e_ref, fx_ref, fy_ref, fz_ref, mid_ref, p_ref, r_ref, q_ref, x_ref, acc_ref, norm_ref, *, dims):
    n_m, n_s, held, bx, by, n_obs = dims
    nx, ny = n_s * bx, n_m * by
    nz = g_ref.shape[1]
    block = bx * by
    rows = (held + 1) * block + n_obs
    plane = (ny, nz)
    lane = lax.broadcasted_iota(jnp.int32, plane, 1)
    sub = lax.broadcasted_iota(jnp.int32, plane, 0)

    def at(j, x, shift=0):
        start = pl.multiple_of((j * nx + x) * ny, ny)
        return pl.ds(start + (TILE + shift), ny)

    def member(j):
        return pl.ds(pl.multiple_of(j * ny, ny), ny)

    def for_members(fn, unroll=1):
        def body(j, carry):
            fn(j)
            return carry

        lax.fori_loop(0, held, body, 0, unroll=unroll)

    for ref in (p_ref, fy_ref):
        for edge in (0, TILE + held * nx * ny):
            ref[pl.ds(edge, TILE), :] = jnp.zeros((TILE, nz), jnp.float32)

    for m in range(n_m):
        for s in range(n_s):
            base = (m * n_s + s) * rows
            for a in range(bx):
                x = s * bx + a
                for j in range(held):
                    e_ref[pl.ds(TILE + (j * nx + x) * ny + m * by, by), :] = g_ref[
                        pl.ds(base + j * block + a * by, by), :
                    ]
                x_ref[pl.ds(TILE + x * ny + m * by, by), :] = g_ref[pl.ds(base + held * block + a * by, by), :]

    norm0 = jnp.zeros(plane, jnp.float32)
    for x in range(nx):
        v = x_ref[at(0, x), :]
        norm0 = norm0 + v * v
        for j in range(held):
            p_ref[at(j, x), :] = v
            r_ref[at(j, x), :] = v
    norm0 = jnp.broadcast_to(total(norm0), plane)
    for j in range(held):
        norm_ref[member(j), :] = norm0
    x_ref[...] = jnp.zeros(x_ref.shape, jnp.float32)

    edge_z = (lane == 0).astype(jnp.float32) + (lane == nz - 1).astype(jnp.float32)
    edge_y = (sub == 0).astype(jnp.float32) + (sub == ny - 1).astype(jnp.float32)

    def faces(j):
        e = jnp.exp(-e_ref[at(j, 0), :])
        fx = None
        for x in range(nx):
            fy = jnp.where(sub > 0, 2.0 / (e + pltpu.roll(e, 1, 0)), 0.0)
            fz = jnp.where(lane > 0, 2.0 / (e + pltpu.roll(e, 1, 1)), 0.0)
            fy_ref[at(j, x), :] = fy
            fz_ref[at(j, x), :] = fz
            mid = (fy + pltpu.roll(fy, ny - 1, 0)) + (fz + pltpu.roll(fz, nz - 1, 1))
            ends = edge_y + edge_z
            if x == 0 or x == nx - 1:
                ends = ends + 1.0
            mid = mid + ends / e
            if fx is not None:
                mid = mid + fx
            if x + 1 < nx:
                after = jnp.exp(-e_ref[at(j, x + 1), :])
                fx = 2.0 / (e + after)
                fx_ref[at(j, x + 1), :] = fx
                mid = mid + fx
                e = after
            mid_ref[at(j, x), :] = mid

    for_members(faces)

    def along_z(j, x, v):
        f = fz_ref[at(j, x), :]
        q_ref[at(j, x), :] = f * pltpu.roll(v, 1, 1) + pltpu.roll(f * v, nz - 1, 1)

    def start(j):
        for x in range(nx):
            along_z(j, x, p_ref[at(j, x), :])

    def apply(j):
        acc = jnp.zeros(plane, jnp.float32)
        before, fx = None, None
        v = p_ref[at(j, 0), :]
        for x in range(nx):
            image = mid_ref[at(j, x), :] * v - q_ref[at(j, x), :]
            image = image - fy_ref[at(j, x), :] * p_ref[at(j, x, -1), :]
            image = image - fy_ref[at(j, x, 1), :] * p_ref[at(j, x, 1), :]
            if x > 0:
                image = image - fx * before
            if x + 1 < nx:
                after = p_ref[at(j, x + 1), :]
                fx = fx_ref[at(j, x + 1), :]
                image = image - fx * after
            q_ref[at(j, x), :] = image
            acc = acc + v * image
            if x + 1 < nx:
                before, v = v, after
        acc_ref[member(j), :] = acc

    def totals():
        return [jnp.broadcast_to(total(acc_ref[member(j), :]), plane) for j in range(held)]

    def multiply():
        for_members(apply)
        for j, dot in enumerate(totals()):
            acc_ref[member(j), :] = norm_ref[member(j), :] / dot

    def move(j):
        step = acc_ref[member(j), :]
        acc = jnp.zeros(plane, jnp.float32)
        for x in range(nx):
            x_ref[at(j, x), :] = x_ref[at(j, x), :] + step * p_ref[at(j, x), :]
            res = r_ref[at(j, x), :] - step * q_ref[at(j, x), :]
            r_ref[at(j, x), :] = res
            acc = acc + res * res
        acc_ref[member(j), :] = acc

    def turn(j):
        ratio = acc_ref[member(j), :]
        for x in range(nx):
            v = r_ref[at(j, x), :] + ratio * p_ref[at(j, x), :]
            p_ref[at(j, x), :] = v
            along_z(j, x, v)

    def one(iteration, carry):
        multiply()
        for_members(move)
        for j, norm in enumerate(totals()):
            acc_ref[member(j), :] = norm / norm_ref[member(j), :]
            norm_ref[member(j), :] = norm
        for_members(turn, UNROLL)
        return carry

    for_members(start, UNROLL)
    lax.fori_loop(0, ITERS - 1, one, 0)
    multiply()

    for m in range(n_m):
        for s in range(n_s):
            peer = m * n_s + s
            for o in range(n_obs):
                picked = g_ref[pl.ds(peer * rows + (held + 1) * block + o, 1), :].astype(jnp.int32)[0, 0]
                cell = (s * bx + picked // by) * ny + m * by + picked % by
                for j in range(held):
                    row = pl.ds(TILE + j * nx * ny + cell, 1)
                    out_ref[pl.ds((peer * held + j) * n_obs + o, 1), :] = (
                        x_ref[row, :] + acc_ref[pl.ds(j * ny, 1), :] * p_ref[row, :]
                    )


def sums_kernel(pred_ref, values_ref, noise_ref, var_ref, out_ref, *, devices):
    members = pred_ref.shape[0]
    held = members // devices
    pred = pred_ref[...]
    inv_sigma = 1.0 / jnp.sqrt(var_ref[...])
    mean = jnp.sum(pred, axis=0, keepdims=True) / members
    spread = (pred - mean) * inv_sigma
    misfit = (values_ref[...] - pred) * inv_sigma + noise_ref[...]
    by_last = (((1,), (1,)), ((), ()))
    gram = lax.dot_general(spread, spread, by_last, precision=HIGHEST, preferred_element_type=jnp.float32)
    cross = lax.dot_general(spread, misfit, by_last, precision=HIGHEST, preferred_element_type=jnp.float32)
    for d in range(devices):
        out_ref[d, 0:held, :] = gram[d * held : (d + 1) * held, :]
        out_ref[d, held : 2 * held, :] = cross[d * held : (d + 1) * held, :]


def spread_kernel(parts_ref, out_ref):
    devices = parts_ref.shape[0]
    own = jnp.sum(parts_ref[...], axis=0)
    for d in range(devices):
        out_ref[d] = own


def update_kernel(sums_ref, field_ref, found_ref, out_ref, predicted_ref, a_ref, c_ref, sem, *, devices):
    predicted = pltpu.make_async_copy(found_ref, predicted_ref, sem)
    predicted.start()
    members = sums_ref.shape[2]
    held = members // devices
    tile = 8
    for d in range(devices):
        a_ref[pl.ds(d * held, held), :] = sums_ref[d, 0:held, :]
        c_ref[pl.ds(d * held, held), :] = sums_ref[d, held : 2 * held, :]
    lane = lax.broadcasted_iota(jnp.int32, (tile, members), 1)
    sub = lax.broadcasted_iota(jnp.int32, (tile, members), 0)
    blocks = members // tile
    left, right = [], []
    for k in range(blocks):
        own = (lane == sub + k * tile).astype(jnp.float32) * (members - 1.0)
        left.append(a_ref[pl.ds(k * tile, tile), :] + own)
        right.append(c_ref[pl.ds(k * tile, tile), :])
    wide = (tile, members)

    def row(x, t):
        return jnp.broadcast_to(x[t : t + 1, :], wide)

    def column(x, t):
        return jnp.broadcast_to(x[:, t : t + 1], wide)

    for k in range(blocks):
        parts = [column(left[k], k * tile + t) for t in range(tile)] + [left[k], right[k]]
        for t in range(tile):
            inverse = 1.0 / row(parts[t], t)
            factor = jnp.where(sub == t, 0.0, parts[t] * inverse)
            scaled = sub == t
            for i in range(t + 1, len(parts)):
                pivot = row(parts[i], t)
                parts[i] = jnp.where(scaled, pivot * inverse, parts[i] - factor * pivot)
        left[k], right[k] = parts[-2], parts[-1]
        rows_left = [row(left[k], t) for t in range(tile)]
        rows_right = [row(right[k], t) for t in range(tile)]
        for i in range(blocks):
            if i != k:
                columns = [column(left[i], k * tile + t) for t in range(tile)]
                for t in range(tile):
                    right[i] = right[i] - columns[t] * rows_right[t]
                    if k + 1 < blocks:
                        left[i] = left[i] - columns[t] * rows_left[t]
    for k in range(blocks):
        c_ref[pl.ds(k * tile, tile), :] = right[k]
    weights = c_ref[...]
    cells = field_ref.shape[0] // members
    by_first = (((0,), (0,)), ((), ()))
    for c in range(cells):
        field = field_ref[pl.ds(c, members, stride=cells), :]
        anomaly = field - jnp.sum(field, axis=0, keepdims=True) / members
        moved = lax.dot_general(weights, anomaly, by_first, precision=HIGHEST, preferred_element_type=jnp.float32)
        out_ref[pl.ds(c, members, stride=cells), :] = field + moved
    predicted.wait()


def exchange(x):
    return lax.all_to_all(x, AXES, split_axis=0, concat_axis=0, tiled=True)


def local_whole(ensemble, source, obs_rows, obs_values, obs_noise, obs_var):
    members = ensemble.shape[0]
    bx, by, nz = source.shape
    n_m, n_s = lax.axis_size("member"), lax.axis_size("space")
    devices = n_m * n_s
    held = members // devices
    block = bx * by
    n_obs = obs_rows.shape[-1]
    rows = (held + 1) * block + n_obs
    packed = vmem_call(
        pack_kernel,
        pltpu.VMEM((devices, rows, 1, nz), jnp.float32),
        [
            pltpu.VMEM((block, 1, nz), jnp.float32),
            pltpu.SMEM((n_obs,), jnp.int32),
            pltpu.SemaphoreType.DMA((3,)),
        ],
        "pack",
        ensemble.reshape(devices, held * block, 1, nz),
        source.reshape(block, 1, nz),
        obs_rows.reshape(-1),
        spaces=[pl.ANY] * 3,
    )
    got = exchange(packed.reshape(devices * rows, 1, nz)).reshape(devices * rows, nz)
    nx, ny = n_s * bx, n_m * by
    field = pltpu.VMEM((held * nx * ny + 2 * TILE, nz), jnp.float32)
    plane = pltpu.VMEM((held * ny, nz), jnp.float32)
    picked = vmem_call(
        functools.partial(pressure_kernel, dims=(n_m, n_s, held, bx, by, n_obs)),
        pltpu.VMEM((members * n_obs, nz), jnp.float32),
        [field] * 9 + [plane] * 2,
        "pressure",
        near(got),
    )
    returned = exchange(picked.reshape(members * n_obs, 1, nz))
    sums = vmem_call(
        functools.partial(sums_kernel, devices=devices),
        pltpu.VMEM((devices, 2 * held, members), jnp.float32),
        [],
        "sums",
        near(returned.reshape(members, n_obs * nz)),
        obs_values.reshape(1, -1),
        near(obs_noise.reshape(members, -1)),
        obs_var.reshape(1, -1),
    )
    own = vmem_call(spread_kernel, pltpu.VMEM(sums.shape, jnp.float32), [], "spread", near(exchange(sums)))
    gathered = exchange(own)
    updated, predicted = vmem_call(
        functools.partial(update_kernel, devices=devices),
        [
            jax.ShapeDtypeStruct((members * block, nz), jnp.float32),
            jax.ShapeDtypeStruct((members, n_obs * nz), jnp.float32),
        ],
        [pltpu.VMEM((members, members), jnp.float32)] * 2 + [pltpu.SemaphoreType.DMA],
        "update",
        near(gathered),
        near(ensemble.reshape(members * block, nz)),
        near(returned.reshape(members, n_obs * nz)),
        outs=[pl.BlockSpec(memory_space=pltpu.VMEM), pl.BlockSpec(memory_space=pl.ANY)],
    )
    return (updated.reshape(ensemble.shape), predicted.reshape(members, 1, 1, n_obs * nz))


def local(ensemble, *rest):
    devices = lax.axis_size("member") * lax.axis_size("space")
    form = local_whole if ensemble.shape[0] % devices == 0 else local_split
    return form(ensemble, *rest)


def solution(mesh):
    in_specs = (
        P(None, "space", "member", None),
        P("space", "member", None),
        P("space", "member", None),
        P("space", "member", None),
        P(None, "space", "member", None),
        P("space", "member", None),
    )
    out_specs = (P(None, "space", "member", None), P(None, "space", "member", None))
    return jax.shard_map(local, mesh=mesh, in_specs=in_specs, out_specs=out_specs, check_vma=False)
```

```python
import functools

import jax
import jax.numpy as jnp
from jax import lax
from jax.experimental import pallas as pl
from jax.experimental.pallas import tpu as pltpu
from jax.sharding import PartitionSpec as P

ITERS = 4
TILE = 8
AXES = ("member", "space")
HIGHEST = lax.Precision.HIGHEST


def padded_2(x, sides, width):
    for axis, dim in sides:
        devices, length = (lax.axis_size(axis), x.shape[dim])
        up = [(i, (i + 1) % devices) for i in range(devices - 1)]
        down = [(j, i) for i, j in up]
        last = lax.slice_in_dim(x, length - width, length, axis=dim)
        leading = lax.slice_in_dim(x, 0, width, axis=dim)
        before = lax.ppermute(last, axis, up)
        after = lax.ppermute(leading, axis, down)
        x = jnp.concatenate([before, x, after], axis=dim)
    return x


def harmonic(first_cond, second_cond):
    return 2.0 * first_cond * second_cond / (first_cond + second_cond)


def extend(values_in):
    widened = padded_2(values_in, (("member", 2),), 1)
    return jnp.pad(widened, ((0, 0), (1, 1), (0, 0), (1, 1)))


def member_dots(dot_terms):
    return lax.psum(dot_terms, "member")


def face_terms(cond):
    widened = extend(cond)
    edge_pad = jnp.pad(cond, ((0, 0), (1, 1), (1, 1), (1, 1)), mode="edge")
    cond_pad = jnp.where(widened > 0.0, widened, edge_pad)
    face_x = harmonic(cond_pad[:, :-1, 1:-1, 1:-1], cond_pad[:, 1:, 1:-1, 1:-1])
    face_y = harmonic(cond_pad[:, 1:-1, :-1, 1:-1], cond_pad[:, 1:-1, 1:, 1:-1])
    face_z = harmonic(cond, cond_pad[:, 1:-1, 1:-1, 2:])
    lower_z = jnp.concatenate([harmonic(cond[..., :1], cond[..., :1]), face_z[..., :-1]], axis=-1)
    return (face_x, face_y, face_z, lower_z)


def operate(values_in, face_x, face_y, face_z, lower_z):
    padded = extend(values_in)
    result = face_x[:, 1:] * (values_in - padded[:, 2:, 1:-1, 1:-1]) + face_x[:, :-1] * (
        values_in - padded[:, :-2, 1:-1, 1:-1]
    )
    result = (
        result
        + face_y[:, :, 1:] * (values_in - padded[:, 1:-1, 2:, 1:-1])
        + face_y[:, :, :-1] * (values_in - padded[:, 1:-1, :-2, 1:-1])
    )
    result = (
        result
        + face_z * (values_in - padded[:, 1:-1, 1:-1, 2:])
        + lower_z * (values_in - padded[:, 1:-1, 1:-1, :-2])
    )
    return result


def conjugate(cond, forcing):
    face_x, face_y, face_z, lower_z = face_terms(cond)
    residual = jnp.broadcast_to(forcing[None], cond.shape)
    direction = residual
    solution = jnp.zeros_like(cond)
    norm_now = member_dots(jnp.sum(residual * residual, axis=(1, 2, 3)))
    for iteration in range(ITERS):
        image = operate(direction, face_x, face_y, face_z, lower_z)
        step_size = norm_now / member_dots(jnp.sum(direction * image, axis=(1, 2, 3)))
        solution = solution + step_size[:, None, None, None] * direction
        residual = residual - step_size[:, None, None, None] * image
        if iteration + 1 < ITERS:
            norm_next = member_dots(jnp.sum(residual * residual, axis=(1, 2, 3)))
            direction = residual + (norm_next / norm_now)[:, None, None, None] * direction
            norm_now = norm_next
    return solution


def local_split(ensemble, source, obs_rows, obs_values, obs_noise, obs_var):
    total_members = ensemble.shape[0]
    block_x, block_y, layers = source.shape
    held_fields = lax.all_to_all(ensemble, "space", split_axis=0, concat_axis=1, tiled=True)
    forcing = lax.all_gather(source, "space", axis=0, tiled=True)
    pressure = conjugate(jnp.exp(held_fields), forcing)
    held_count = pressure.shape[0]
    cells_flat = pressure.reshape(held_count, -1, layers)
    gathered_rows = lax.all_gather(obs_rows, "space", axis=0, tiled=True)
    row_ids = gathered_rows[:, 0]
    peer_ids = jnp.arange(row_ids.shape[0], dtype=jnp.int32)[:, None]
    flat_index = (peer_ids * block_x + row_ids // block_y) * block_y + row_ids % block_y
    picked = jnp.take(cells_flat, flat_index.reshape(-1), axis=1)
    returned = lax.all_to_all(picked, "space", split_axis=1, concat_axis=0, tiled=True)
    predicted = returned.reshape(total_members, 1, 1, -1)
    flat_pred = returned.reshape(total_members, -1)
    inv_sigma = 1.0 / jnp.sqrt(obs_var.reshape(-1))
    spread = (flat_pred - jnp.mean(flat_pred, axis=0)) * inv_sigma
    misfit = (obs_values.reshape(-1) - flat_pred) * inv_sigma + obs_noise.reshape(total_members, -1)
    gram_part = jnp.dot(spread, spread.T, precision=HIGHEST)
    cross_part = jnp.dot(spread, misfit.T, precision=HIGHEST)
    gram_sum, cross_sum = lax.psum((gram_part, cross_part), AXES)
    factor = jnp.linalg.cholesky(
        gram_sum + (total_members - 1.0) * jnp.eye(total_members, dtype=jnp.float32)
    )
    weights = jax.scipy.linalg.cho_solve((factor, True), cross_sum)
    flat_field = ensemble.reshape(total_members, -1)
    anomalies = flat_field - jnp.mean(flat_field, axis=0)
    updated = flat_field + jnp.dot(weights.T, anomalies, precision=HIGHEST)
    return (updated.reshape(ensemble.shape), predicted)


def vmem_call(kernel, out, scratch, name, *operands, spaces=None, outs=pl.BlockSpec(memory_space=pltpu.VMEM)):
    specs = [pl.BlockSpec(memory_space=s) for s in spaces or [pltpu.VMEM] * len(operands)]
    return pl.pallas_call(
        kernel,
        out_shape=out,
        in_specs=specs,
        out_specs=outs,
        scratch_shapes=scratch,
        name=name,
    )(*operands)


def near(x):
    return pltpu.with_memory_space_constraint(x, pltpu.VMEM)


def pack_kernel(field_ref, source_ref, obs_ref, out_ref, block_ref, rows_ref, sems):
    devices, _, _, nz = out_ref.shape
    cells, block, n_obs = field_ref.shape[1], source_ref.shape[0], obs_ref.shape[0]
    fields = pltpu.make_async_copy(field_ref, out_ref.at[:, pl.ds(0, cells)], sems.at[0])
    source = pltpu.make_async_copy(source_ref, block_ref, sems.at[1])
    rows = pltpu.make_async_copy(obs_ref, rows_ref, sems.at[2])
    rows.start()
    source.start()
    fields.start()
    rows.wait()
    for o in range(n_obs):
        pick = jnp.full((1, 1, nz), rows_ref[o].astype(jnp.float32))
        for d in range(devices):
            out_ref[d, pl.ds(cells + block + o, 1)] = pick
    source.wait()
    held = block_ref[...]
    for d in range(devices):
        out_ref[d, pl.ds(cells, block)] = held
    fields.wait()


def total(acc):
    return jnp.sum(jnp.sum(acc, axis=0, keepdims=True), axis=1, keepdims=True)


def pressure_kernel(g_ref, out_ref, e_ref, fx_ref, fy_ref, fz_ref, mid_ref, p_ref, r_ref, q_ref, x_ref, acc_ref, norm_ref, *, dims):
    n_m, n_s, held, bx, by, n_obs = dims
    nx, ny = n_s * bx, n_m * by
    nz = g_ref.shape[1]
    block = bx * by
    rows = (held + 1) * block + n_obs
    plane = (ny, nz)
    lane = lax.broadcasted_iota(jnp.int32, plane, 1)
    sub = lax.broadcasted_iota(jnp.int32, plane, 0)

    def at(j, x, shift=0):
        start = pl.multiple_of((j * nx + x) * ny, ny)
        return pl.ds(start + (TILE + shift), ny)

    def member(j):
        return pl.ds(pl.multiple_of(j * ny, ny), ny)

    def for_members(fn):
        def body(j, carry):
            fn(j)
            return carry

        lax.fori_loop(0, held, body, 0)

    for ref in (p_ref, fy_ref):
        for edge in (0, TILE + held * nx * ny):
            ref[pl.ds(edge, TILE), :] = jnp.zeros((TILE, nz), jnp.float32)

    for m in range(n_m):
        for s in range(n_s):
            base = (m * n_s + s) * rows
            for a in range(bx):
                x = s * bx + a
                for j in range(held):
                    e_ref[pl.ds(TILE + (j * nx + x) * ny + m * by, by), :] = g_ref[
                        pl.ds(base + j * block + a * by, by), :
                    ]
                x_ref[pl.ds(TILE + x * ny + m * by, by), :] = g_ref[pl.ds(base + held * block + a * by, by), :]

    norm0 = jnp.zeros(plane, jnp.float32)
    for x in range(nx):
        v = x_ref[at(0, x), :]
        norm0 = norm0 + v * v
        for j in range(held):
            p_ref[at(j, x), :] = v
            r_ref[at(j, x), :] = v
    norm0 = jnp.broadcast_to(total(norm0), plane)
    for j in range(held):
        norm_ref[member(j), :] = norm0
    x_ref[...] = jnp.zeros(x_ref.shape, jnp.float32)

    edge_z = (lane == 0).astype(jnp.float32) + (lane == nz - 1).astype(jnp.float32)
    edge_y = (sub == 0).astype(jnp.float32) + (sub == ny - 1).astype(jnp.float32)

    def faces(j):
        e = jnp.exp(-e_ref[at(j, 0), :])
        fx = None
        for x in range(nx):
            fy = jnp.where(sub > 0, 2.0 / (e + pltpu.roll(e, 1, 0)), 0.0)
            fz = jnp.where(lane > 0, 2.0 / (e + pltpu.roll(e, 1, 1)), 0.0)
            fy_ref[at(j, x), :] = fy
            fz_ref[at(j, x), :] = fz
            mid = (fy + pltpu.roll(fy, ny - 1, 0)) + (fz + pltpu.roll(fz, nz - 1, 1))
            ends = edge_y + edge_z
            if x == 0 or x == nx - 1:
                ends = ends + 1.0
            mid = mid + ends / e
            if fx is not None:
                mid = mid + fx
            if x + 1 < nx:
                after = jnp.exp(-e_ref[at(j, x + 1), :])
                fx = 2.0 / (e + after)
                fx_ref[at(j, x + 1), :] = fx
                mid = mid + fx
                e = after
            mid_ref[at(j, x), :] = mid

    for_members(faces)

    def turn(j, ratio):
        for x in range(nx):
            v = r_ref[at(j, x), :] + ratio * p_ref[at(j, x), :]
            p_ref[at(j, x), :] = v
            f = fz_ref[at(j, x), :]
            q_ref[at(j, x), :] = f * pltpu.roll(v, 1, 1) + pltpu.roll(f * v, nz - 1, 1)
            yield

    def apply(j, dots):
        acc = jnp.zeros(plane, jnp.float32)
        before, fx = None, None
        v = p_ref[at(j, 0), :]
        for x in range(nx):
            image = mid_ref[at(j, x), :] * v - q_ref[at(j, x), :]
            image = image - fy_ref[at(j, x), :] * p_ref[at(j, x, -1), :]
            image = image - fy_ref[at(j, x, 1), :] * p_ref[at(j, x, 1), :]
            if x > 0:
                image = image - fx * before
            if x + 1 < nx:
                after = p_ref[at(j, x + 1), :]
                fx = fx_ref[at(j, x + 1), :]
                image = image - fx * after
            q_ref[at(j, x), :] = image
            acc = acc + v * image
            if x + 1 < nx:
                before, v = v, after
            yield
        dots[j] = acc

    def move(j, step, norms):
        acc = jnp.zeros(plane, jnp.float32)
        for x in range(nx):
            x_ref[at(j, x), :] = x_ref[at(j, x), :] + step * p_ref[at(j, x), :]
            res = r_ref[at(j, x), :] - step * q_ref[at(j, x), :]
            r_ref[at(j, x), :] = res
            acc = acc + res * res
            yield
        norms[j] = acc

    def together(*stages):
        stages = list(stages)
        while stages:
            stages = [stage for stage in stages if next(stage, stage) is not stage]

    def spread_total(acc):
        return jnp.broadcast_to(total(acc), plane)

    def steps_of(dots):
        return {j: norm_ref[member(j), :] / spread_total(dot) for j, dot in dots.items()}

    def ratios_of(norms):
        ratios = {}
        for j, norm in norms.items():
            norm = spread_total(norm)
            ratios[j] = norm / norm_ref[member(j), :]
            norm_ref[member(j), :] = norm
        return ratios

    ahead, behind = range(held // 2), range(held // 2, held)

    def open_stage():
        dots = {}
        together(*[apply(j, dots) for j in ahead], *[turn(j, acc_ref[member(j), :]) for j in behind])
        return steps_of(dots)

    def one(iteration, carry):
        steps, dots, norms = open_stage(), {}, {}
        together(*[apply(j, dots) for j in behind], *[move(j, steps[j], norms) for j in ahead])
        ratios, steps, norms = ratios_of(norms), steps_of(dots), {}
        together(*[turn(j, ratios[j]) for j in ahead], *[move(j, steps[j], norms) for j in behind])
        for j, ratio in ratios_of(norms).items():
            acc_ref[member(j), :] = ratio
        return carry

    acc_ref[...] = jnp.zeros(acc_ref.shape, jnp.float32)
    together(*[turn(j, acc_ref[member(j), :]) for j in ahead])
    lax.fori_loop(0, ITERS - 1, one, 0)
    steps, dots = open_stage(), {}
    together(*[apply(j, dots) for j in behind])
    steps.update(steps_of(dots))
    for j, step in steps.items():
        acc_ref[member(j), :] = step

    for m in range(n_m):
        for s in range(n_s):
            peer = m * n_s + s
            for o in range(n_obs):
                picked = g_ref[pl.ds(peer * rows + (held + 1) * block + o, 1), :].astype(jnp.int32)[0, 0]
                cell = (s * bx + picked // by) * ny + m * by + picked % by
                for j in range(held):
                    row = pl.ds(TILE + j * nx * ny + cell, 1)
                    out_ref[pl.ds((peer * held + j) * n_obs + o, 1), :] = (
                        x_ref[row, :] + acc_ref[pl.ds(j * ny, 1), :] * p_ref[row, :]
                    )


def sums_kernel(pred_ref, values_ref, noise_ref, var_ref, out_ref, *, devices):
    members = pred_ref.shape[0]
    held = members // devices
    pred = pred_ref[...]
    inv_sigma = 1.0 / jnp.sqrt(var_ref[...])
    mean = jnp.sum(pred, axis=0, keepdims=True) / members
    spread = (pred - mean) * inv_sigma
    misfit = (values_ref[...] - pred) * inv_sigma + noise_ref[...]
    by_last = (((1,), (1,)), ((), ()))
    gram = lax.dot_general(spread, spread, by_last, precision=HIGHEST, preferred_element_type=jnp.float32)
    cross = lax.dot_general(spread, misfit, by_last, precision=HIGHEST, preferred_element_type=jnp.float32)
    for d in range(devices):
        out_ref[d, 0:held, :] = gram[d * held : (d + 1) * held, :]
        out_ref[d, held : 2 * held, :] = cross[d * held : (d + 1) * held, :]


def spread_kernel(parts_ref, out_ref):
    devices = parts_ref.shape[0]
    own = jnp.sum(parts_ref[...], axis=0)
    for d in range(devices):
        out_ref[d] = own


def update_kernel(sums_ref, field_ref, found_ref, out_ref, predicted_ref, a_ref, c_ref, sem, *, devices):
    predicted = pltpu.make_async_copy(found_ref, predicted_ref, sem)
    predicted.start()
    members = sums_ref.shape[2]
    held = members // devices
    tile = 8
    for d in range(devices):
        a_ref[pl.ds(d * held, held), :] = sums_ref[d, 0:held, :]
        c_ref[pl.ds(d * held, held), :] = sums_ref[d, held : 2 * held, :]
    lane = lax.broadcasted_iota(jnp.int32, (tile, members), 1)
    sub = lax.broadcasted_iota(jnp.int32, (tile, members), 0)
    blocks = members // tile
    left, right = [], []
    for k in range(blocks):
        own = (lane == sub + k * tile).astype(jnp.float32) * (members - 1.0)
        left.append(a_ref[pl.ds(k * tile, tile), :] + own)
        right.append(c_ref[pl.ds(k * tile, tile), :])
    wide = (tile, members)

    def row(x, t):
        return jnp.broadcast_to(x[t : t + 1, :], wide)

    def column(x, t):
        return jnp.broadcast_to(x[:, t : t + 1], wide)

    for k in range(blocks):
        parts = [column(left[k], k * tile + t) for t in range(tile)] + [left[k], right[k]]
        for t in range(tile):
            inverse = 1.0 / row(parts[t], t)
            factor = jnp.where(sub == t, 0.0, parts[t] * inverse)
            scaled = sub == t
            for i in range(t + 1, len(parts)):
                pivot = row(parts[i], t)
                parts[i] = jnp.where(scaled, pivot * inverse, parts[i] - factor * pivot)
        left[k], right[k] = parts[-2], parts[-1]
        rows_left = [row(left[k], t) for t in range(tile)]
        rows_right = [row(right[k], t) for t in range(tile)]
        for i in range(blocks):
            if i != k:
                columns = [column(left[i], k * tile + t) for t in range(tile)]
                for t in range(tile):
                    right[i] = right[i] - columns[t] * rows_right[t]
                    if k + 1 < blocks:
                        left[i] = left[i] - columns[t] * rows_left[t]
    for k in range(blocks):
        c_ref[pl.ds(k * tile, tile), :] = right[k]
    weights = c_ref[...]
    cells = field_ref.shape[0] // members
    by_first = (((0,), (0,)), ((), ()))
    for c in range(cells):
        field = field_ref[pl.ds(c, members, stride=cells), :]
        anomaly = field - jnp.sum(field, axis=0, keepdims=True) / members
        moved = lax.dot_general(weights, anomaly, by_first, precision=HIGHEST, preferred_element_type=jnp.float32)
        out_ref[pl.ds(c, members, stride=cells), :] = field + moved
    predicted.wait()


def exchange(x):
    return lax.all_to_all(x, AXES, split_axis=0, concat_axis=0, tiled=True)


def local_whole(ensemble, source, obs_rows, obs_values, obs_noise, obs_var):
    members = ensemble.shape[0]
    bx, by, nz = source.shape
    n_m, n_s = lax.axis_size("member"), lax.axis_size("space")
    devices = n_m * n_s
    held = members // devices
    block = bx * by
    n_obs = obs_rows.shape[-1]
    rows = (held + 1) * block + n_obs
    packed = vmem_call(
        pack_kernel,
        pltpu.VMEM((devices, rows, 1, nz), jnp.float32),
        [
            pltpu.VMEM((block, 1, nz), jnp.float32),
            pltpu.SMEM((n_obs,), jnp.int32),
            pltpu.SemaphoreType.DMA((3,)),
        ],
        "pack",
        ensemble.reshape(devices, held * block, 1, nz),
        source.reshape(block, 1, nz),
        obs_rows.reshape(-1),
        spaces=[pl.ANY] * 3,
    )
    got = exchange(packed.reshape(devices * rows, 1, nz)).reshape(devices * rows, nz)
    nx, ny = n_s * bx, n_m * by
    field = pltpu.VMEM((held * nx * ny + 2 * TILE, nz), jnp.float32)
    plane = pltpu.VMEM((held * ny, nz), jnp.float32)
    picked = vmem_call(
        functools.partial(pressure_kernel, dims=(n_m, n_s, held, bx, by, n_obs)),
        pltpu.VMEM((members * n_obs, nz), jnp.float32),
        [field] * 9 + [plane] * 2,
        "pressure",
        near(got),
    )
    returned = exchange(picked.reshape(members * n_obs, 1, nz))
    sums = vmem_call(
        functools.partial(sums_kernel, devices=devices),
        pltpu.VMEM((devices, 2 * held, members), jnp.float32),
        [],
        "sums",
        near(returned.reshape(members, n_obs * nz)),
        obs_values.reshape(1, -1),
        near(obs_noise.reshape(members, -1)),
        obs_var.reshape(1, -1),
    )
    own = vmem_call(spread_kernel, pltpu.VMEM(sums.shape, jnp.float32), [], "spread", near(exchange(sums)))
    gathered = exchange(own)
    updated, predicted = vmem_call(
        functools.partial(update_kernel, devices=devices),
        [
            jax.ShapeDtypeStruct((members * block, nz), jnp.float32),
            jax.ShapeDtypeStruct((members, n_obs * nz), jnp.float32),
        ],
        [pltpu.VMEM((members, members), jnp.float32)] * 2 + [pltpu.SemaphoreType.DMA],
        "update",
        near(gathered),
        near(ensemble.reshape(members * block, nz)),
        near(returned.reshape(members, n_obs * nz)),
        outs=[pl.BlockSpec(memory_space=pltpu.VMEM), pl.BlockSpec(memory_space=pl.ANY)],
    )
    return (updated.reshape(ensemble.shape), predicted.reshape(members, 1, 1, n_obs * nz))


def local(ensemble, *rest):
    devices = lax.axis_size("member") * lax.axis_size("space")
    form = local_whole if ensemble.shape[0] % devices == 0 else local_split
    return form(ensemble, *rest)


def solution(mesh):
    in_specs = (
        P(None, "space", "member", None),
        P("space", "member", None),
        P("space", "member", None),
        P("space", "member", None),
        P(None, "space", "member", None),
        P("space", "member", None),
    )
    out_specs = (P(None, "space", "member", None), P(None, "space", "member", None))
    return jax.shard_map(local, mesh=mesh, in_specs=in_specs, out_specs=out_specs, check_vma=False)
```

```python
import functools

import jax
import jax.numpy as jnp
from jax import lax
from jax.experimental import pallas as pl
from jax.experimental.pallas import tpu as pltpu
from jax.sharding import PartitionSpec as P

ITERS = 4
TILE = 8
AXES = ("member", "space")
HIGHEST = lax.Precision.HIGHEST


def padded_2(x, sides, width):
    for axis, dim in sides:
        devices, length = (lax.axis_size(axis), x.shape[dim])
        up = [(i, (i + 1) % devices) for i in range(devices - 1)]
        down = [(j, i) for i, j in up]
        last = lax.slice_in_dim(x, length - width, length, axis=dim)
        leading = lax.slice_in_dim(x, 0, width, axis=dim)
        before = lax.ppermute(last, axis, up)
        after = lax.ppermute(leading, axis, down)
        x = jnp.concatenate([before, x, after], axis=dim)
    return x


def harmonic(first_cond, second_cond):
    return 2.0 * first_cond * second_cond / (first_cond + second_cond)


def extend(values_in):
    widened = padded_2(values_in, (("member", 2),), 1)
    return jnp.pad(widened, ((0, 0), (1, 1), (0, 0), (1, 1)))


def member_dots(dot_terms):
    return lax.psum(dot_terms, "member")


def face_terms(cond):
    widened = extend(cond)
    edge_pad = jnp.pad(cond, ((0, 0), (1, 1), (1, 1), (1, 1)), mode="edge")
    cond_pad = jnp.where(widened > 0.0, widened, edge_pad)
    face_x = harmonic(cond_pad[:, :-1, 1:-1, 1:-1], cond_pad[:, 1:, 1:-1, 1:-1])
    face_y = harmonic(cond_pad[:, 1:-1, :-1, 1:-1], cond_pad[:, 1:-1, 1:, 1:-1])
    face_z = harmonic(cond, cond_pad[:, 1:-1, 1:-1, 2:])
    lower_z = jnp.concatenate([harmonic(cond[..., :1], cond[..., :1]), face_z[..., :-1]], axis=-1)
    return (face_x, face_y, face_z, lower_z)


def operate(values_in, face_x, face_y, face_z, lower_z):
    padded = extend(values_in)
    result = face_x[:, 1:] * (values_in - padded[:, 2:, 1:-1, 1:-1]) + face_x[:, :-1] * (
        values_in - padded[:, :-2, 1:-1, 1:-1]
    )
    result = (
        result
        + face_y[:, :, 1:] * (values_in - padded[:, 1:-1, 2:, 1:-1])
        + face_y[:, :, :-1] * (values_in - padded[:, 1:-1, :-2, 1:-1])
    )
    result = (
        result
        + face_z * (values_in - padded[:, 1:-1, 1:-1, 2:])
        + lower_z * (values_in - padded[:, 1:-1, 1:-1, :-2])
    )
    return result


def conjugate(cond, forcing):
    face_x, face_y, face_z, lower_z = face_terms(cond)
    residual = jnp.broadcast_to(forcing[None], cond.shape)
    direction = residual
    solution = jnp.zeros_like(cond)
    norm_now = member_dots(jnp.sum(residual * residual, axis=(1, 2, 3)))
    for iteration in range(ITERS):
        image = operate(direction, face_x, face_y, face_z, lower_z)
        step_size = norm_now / member_dots(jnp.sum(direction * image, axis=(1, 2, 3)))
        solution = solution + step_size[:, None, None, None] * direction
        residual = residual - step_size[:, None, None, None] * image
        if iteration + 1 < ITERS:
            norm_next = member_dots(jnp.sum(residual * residual, axis=(1, 2, 3)))
            direction = residual + (norm_next / norm_now)[:, None, None, None] * direction
            norm_now = norm_next
    return solution


def local_split(ensemble, source, obs_rows, obs_values, obs_noise, obs_var):
    total_members = ensemble.shape[0]
    block_x, block_y, layers = source.shape
    held_fields = lax.all_to_all(ensemble, "space", split_axis=0, concat_axis=1, tiled=True)
    forcing = lax.all_gather(source, "space", axis=0, tiled=True)
    pressure = conjugate(jnp.exp(held_fields), forcing)
    held_count = pressure.shape[0]
    cells_flat = pressure.reshape(held_count, -1, layers)
    gathered_rows = lax.all_gather(obs_rows, "space", axis=0, tiled=True)
    row_ids = gathered_rows[:, 0]
    peer_ids = jnp.arange(row_ids.shape[0], dtype=jnp.int32)[:, None]
    flat_index = (peer_ids * block_x + row_ids // block_y) * block_y + row_ids % block_y
    picked = jnp.take(cells_flat, flat_index.reshape(-1), axis=1)
    returned = lax.all_to_all(picked, "space", split_axis=1, concat_axis=0, tiled=True)
    predicted = returned.reshape(total_members, 1, 1, -1)
    flat_pred = returned.reshape(total_members, -1)
    inv_sigma = 1.0 / jnp.sqrt(obs_var.reshape(-1))
    spread = (flat_pred - jnp.mean(flat_pred, axis=0)) * inv_sigma
    misfit = (obs_values.reshape(-1) - flat_pred) * inv_sigma + obs_noise.reshape(total_members, -1)
    gram_part = jnp.dot(spread, spread.T, precision=HIGHEST)
    cross_part = jnp.dot(spread, misfit.T, precision=HIGHEST)
    gram_sum, cross_sum = lax.psum((gram_part, cross_part), AXES)
    factor = jnp.linalg.cholesky(
        gram_sum + (total_members - 1.0) * jnp.eye(total_members, dtype=jnp.float32)
    )
    weights = jax.scipy.linalg.cho_solve((factor, True), cross_sum)
    flat_field = ensemble.reshape(total_members, -1)
    anomalies = flat_field - jnp.mean(flat_field, axis=0)
    updated = flat_field + jnp.dot(weights.T, anomalies, precision=HIGHEST)
    return (updated.reshape(ensemble.shape), predicted)


def vmem_call(kernel, out, scratch, name, *operands, spaces=None, outs=pl.BlockSpec(memory_space=pltpu.VMEM)):
    specs = [pl.BlockSpec(memory_space=s) for s in spaces or [pltpu.VMEM] * len(operands)]
    return pl.pallas_call(
        kernel,
        out_shape=out,
        in_specs=specs,
        out_specs=outs,
        scratch_shapes=scratch,
        name=name,
    )(*operands)


def near(x):
    return pltpu.with_memory_space_constraint(x, pltpu.VMEM)


def pack_kernel(field_ref, source_ref, obs_ref, out_ref, block_ref, rows_ref, sems):
    devices, _, _, nz = out_ref.shape
    cells, block, n_obs = field_ref.shape[1], source_ref.shape[0], obs_ref.shape[0]
    fields = pltpu.make_async_copy(field_ref, out_ref.at[:, pl.ds(0, cells)], sems.at[0])
    source = pltpu.make_async_copy(source_ref, block_ref, sems.at[1])
    rows = pltpu.make_async_copy(obs_ref, rows_ref, sems.at[2])
    rows.start()
    source.start()
    fields.start()
    rows.wait()
    for o in range(n_obs):
        pick = jnp.full((1, 1, nz), rows_ref[o].astype(jnp.float32))
        for d in range(devices):
            out_ref[d, pl.ds(cells + block + o, 1)] = pick
    source.wait()
    held = block_ref[...]
    for d in range(devices):
        out_ref[d, pl.ds(cells, block)] = held
    fields.wait()


def total(acc):
    return jnp.sum(jnp.sum(acc, axis=0, keepdims=True), axis=1, keepdims=True)


def pressure_kernel(g_ref, values_hbm, noise_hbm, var_hbm, out_ref, aim_ref, scale_ref, values_ref, var_ref, sems, e_ref, fx_ref, fy_ref, fz_ref, mid_ref, p_ref, r_ref, q_ref, x_ref, acc_ref, norm_ref, *, dims):
    n_m, n_s, held, bx, by, n_obs = dims
    nx, ny = n_s * bx, n_m * by
    nz = g_ref.shape[1]
    block = bx * by
    rows = (held + 1) * block + n_obs
    plane = (ny, nz)
    fetched = ((noise_hbm, aim_ref), (values_hbm, values_ref), (var_hbm, var_ref))
    fetches = [pltpu.make_async_copy(x, y, sems.at[i]) for i, (x, y) in enumerate(fetched)]
    for fetch in fetches:
        fetch.start()
    lane = lax.broadcasted_iota(jnp.int32, plane, 1)
    sub = lax.broadcasted_iota(jnp.int32, plane, 0)

    def at(j, x, shift=0):
        start = pl.multiple_of((j * nx + x) * ny, ny)
        return pl.ds(start + (TILE + shift), ny)

    def member(j):
        return pl.ds(pl.multiple_of(j * ny, ny), ny)

    def for_members(fn):
        def body(j, carry):
            fn(j)
            return carry

        lax.fori_loop(0, held, body, 0)

    for ref in (p_ref, fy_ref):
        for edge in (0, TILE + held * nx * ny):
            ref[pl.ds(edge, TILE), :] = jnp.zeros((TILE, nz), jnp.float32)

    for m in range(n_m):
        for s in range(n_s):
            base = (m * n_s + s) * rows
            for a in range(bx):
                x = s * bx + a
                for j in range(held):
                    e_ref[pl.ds(TILE + (j * nx + x) * ny + m * by, by), :] = g_ref[
                        pl.ds(base + j * block + a * by, by), :
                    ]
                x_ref[pl.ds(TILE + x * ny + m * by, by), :] = g_ref[pl.ds(base + held * block + a * by, by), :]

    norm0 = jnp.zeros(plane, jnp.float32)
    for x in range(nx):
        v = x_ref[at(0, x), :]
        norm0 = norm0 + v * v
        for j in range(held):
            p_ref[at(j, x), :] = v
            r_ref[at(j, x), :] = v
    norm0 = jnp.broadcast_to(total(norm0), plane)
    for j in range(held):
        norm_ref[member(j), :] = norm0
    x_ref[...] = jnp.zeros(x_ref.shape, jnp.float32)

    edge_z = (lane == 0).astype(jnp.float32) + (lane == nz - 1).astype(jnp.float32)
    edge_y = (sub == 0).astype(jnp.float32) + (sub == ny - 1).astype(jnp.float32)

    def faces(j):
        e = jnp.exp(-e_ref[at(j, 0), :])
        fx = None
        for x in range(nx):
            fy = jnp.where(sub > 0, 2.0 / (e + pltpu.roll(e, 1, 0)), 0.0)
            fz = jnp.where(lane > 0, 2.0 / (e + pltpu.roll(e, 1, 1)), 0.0)
            fy_ref[at(j, x), :] = fy
            fz_ref[at(j, x), :] = fz
            mid = (fy + pltpu.roll(fy, ny - 1, 0)) + (fz + pltpu.roll(fz, nz - 1, 1))
            ends = edge_y + edge_z
            if x == 0 or x == nx - 1:
                ends = ends + 1.0
            mid = mid + ends / e
            if fx is not None:
                mid = mid + fx
            if x + 1 < nx:
                after = jnp.exp(-e_ref[at(j, x + 1), :])
                fx = 2.0 / (e + after)
                fx_ref[at(j, x + 1), :] = fx
                mid = mid + fx
                e = after
            mid_ref[at(j, x), :] = mid

    for_members(faces)

    def turn(j, ratio):
        for x in range(nx):
            v = r_ref[at(j, x), :] + ratio * p_ref[at(j, x), :]
            p_ref[at(j, x), :] = v
            f = fz_ref[at(j, x), :]
            q_ref[at(j, x), :] = f * pltpu.roll(v, 1, 1) + pltpu.roll(f * v, nz - 1, 1)
            yield

    def apply(j, dots):
        acc = jnp.zeros(plane, jnp.float32)
        before, fx = None, None
        v = p_ref[at(j, 0), :]
        for x in range(nx):
            image = mid_ref[at(j, x), :] * v - q_ref[at(j, x), :]
            image = image - fy_ref[at(j, x), :] * p_ref[at(j, x, -1), :]
            image = image - fy_ref[at(j, x, 1), :] * p_ref[at(j, x, 1), :]
            if x > 0:
                image = image - fx * before
            if x + 1 < nx:
                after = p_ref[at(j, x + 1), :]
                fx = fx_ref[at(j, x + 1), :]
                image = image - fx * after
            q_ref[at(j, x), :] = image
            acc = acc + v * image
            if x + 1 < nx:
                before, v = v, after
            yield
        dots[j] = acc

    def move(j, step, norms):
        acc = jnp.zeros(plane, jnp.float32)
        for x in range(nx):
            x_ref[at(j, x), :] = x_ref[at(j, x), :] + step * p_ref[at(j, x), :]
            res = r_ref[at(j, x), :] - step * q_ref[at(j, x), :]
            r_ref[at(j, x), :] = res
            acc = acc + res * res
            yield
        norms[j] = acc

    def together(*stages):
        stages = list(stages)
        while stages:
            stages = [stage for stage in stages if next(stage, stage) is not stage]

    def spread_total(acc):
        return jnp.broadcast_to(total(acc), plane)

    def steps_of(dots):
        return {j: norm_ref[member(j), :] / spread_total(dot) for j, dot in dots.items()}

    def ratios_of(norms):
        ratios = {}
        for j, norm in norms.items():
            norm = spread_total(norm)
            ratios[j] = norm / norm_ref[member(j), :]
            norm_ref[member(j), :] = norm
        return ratios

    ahead, behind = range(held // 2), range(held // 2, held)

    def open_stage():
        dots = {}
        together(*[apply(j, dots) for j in ahead], *[turn(j, acc_ref[member(j), :]) for j in behind])
        return steps_of(dots)

    def one(iteration, carry):
        steps, dots, norms = open_stage(), {}, {}
        together(*[apply(j, dots) for j in behind], *[move(j, steps[j], norms) for j in ahead])
        ratios, steps, norms = ratios_of(norms), steps_of(dots), {}
        together(*[turn(j, ratios[j]) for j in ahead], *[move(j, steps[j], norms) for j in behind])
        for j, ratio in ratios_of(norms).items():
            acc_ref[member(j), :] = ratio
        return carry

    acc_ref[...] = jnp.zeros(acc_ref.shape, jnp.float32)
    together(*[turn(j, acc_ref[member(j), :]) for j in ahead])
    lax.fori_loop(0, ITERS - 1, one, 0)
    steps, dots = open_stage(), {}
    together(*[apply(j, dots) for j in behind])
    steps.update(steps_of(dots))
    for j, step in steps.items():
        acc_ref[member(j), :] = step

    for fetch in fetches:
        fetch.wait()
    inv_sigma = 1.0 / jnp.sqrt(var_ref[...])
    scale_ref[...] = inv_sigma
    aim_ref[...] = aim_ref[...] + values_ref[...] * inv_sigma

    for m in range(n_m):
        for s in range(n_s):
            peer = m * n_s + s
            for o in range(n_obs):
                picked = g_ref[pl.ds(peer * rows + (held + 1) * block + o, 1), :].astype(jnp.int32)[0, 0]
                cell = (s * bx + picked // by) * ny + m * by + picked % by
                for j in range(held):
                    row = pl.ds(TILE + j * nx * ny + cell, 1)
                    out_ref[pl.ds((peer * held + j) * n_obs + o, 1), :] = (
                        x_ref[row, :] + acc_ref[pl.ds(j * ny, 1), :] * p_ref[row, :]
                    )


def sums_kernel(pred_ref, aim_ref, scale_ref, out_ref, *, devices):
    members = pred_ref.shape[0]
    held = members // devices
    pred = pred_ref[...]
    inv_sigma = scale_ref[...]
    mean = jnp.sum(pred, axis=0, keepdims=True) / members
    spread = (pred - mean) * inv_sigma
    misfit = aim_ref[...] - pred * inv_sigma
    by_last = (((1,), (1,)), ((), ()))
    gram = lax.dot_general(spread, spread, by_last, precision=HIGHEST, preferred_element_type=jnp.float32)
    cross = lax.dot_general(spread, misfit, by_last, precision=HIGHEST, preferred_element_type=jnp.float32)
    for d in range(devices):
        out_ref[d, 0:held, :] = gram[d * held : (d + 1) * held, :]
        out_ref[d, held : 2 * held, :] = cross[d * held : (d + 1) * held, :]


def spread_kernel(parts_ref, out_ref):
    devices = parts_ref.shape[0]
    own = jnp.sum(parts_ref[...], axis=0)
    for d in range(devices):
        out_ref[d] = own


def update_kernel(sums_ref, field_ref, found_ref, out_ref, predicted_ref, a_ref, c_ref, sem, *, devices):
    predicted = pltpu.make_async_copy(found_ref, predicted_ref, sem)
    predicted.start()
    members = sums_ref.shape[2]
    held = members // devices
    tile = 8
    for d in range(devices):
        a_ref[pl.ds(d * held, held), :] = sums_ref[d, 0:held, :]
        c_ref[pl.ds(d * held, held), :] = sums_ref[d, held : 2 * held, :]
    lane = lax.broadcasted_iota(jnp.int32, (tile, members), 1)
    sub = lax.broadcasted_iota(jnp.int32, (tile, members), 0)
    blocks = members // tile
    left, right = [], []
    for k in range(blocks):
        own = (lane == sub + k * tile).astype(jnp.float32) * (members - 1.0)
        left.append(a_ref[pl.ds(k * tile, tile), :] + own)
        right.append(c_ref[pl.ds(k * tile, tile), :])
    wide = (tile, members)

    def row(x, t):
        return jnp.broadcast_to(x[t : t + 1, :], wide)

    def column(x, t):
        return jnp.broadcast_to(x[:, t : t + 1], wide)

    for k in range(blocks):
        parts = [column(left[k], k * tile + t) for t in range(tile)] + [left[k], right[k]]
        for t in range(tile):
            inverse = 1.0 / row(parts[t], t)
            factor = jnp.where(sub == t, 0.0, parts[t] * inverse)
            scaled = sub == t
            for i in range(t + 1, len(parts)):
                pivot = row(parts[i], t)
                parts[i] = jnp.where(scaled, pivot * inverse, parts[i] - factor * pivot)
        left[k], right[k] = parts[-2], parts[-1]
        rows_left = [row(left[k], t) for t in range(tile)]
        rows_right = [row(right[k], t) for t in range(tile)]
        for i in range(blocks):
            if i != k:
                columns = [column(left[i], k * tile + t) for t in range(tile)]
                for t in range(tile):
                    right[i] = right[i] - columns[t] * rows_right[t]
                    if k + 1 < blocks:
                        left[i] = left[i] - columns[t] * rows_left[t]
    for k in range(blocks):
        c_ref[pl.ds(k * tile, tile), :] = right[k]
    weights = c_ref[...]
    cells = field_ref.shape[0] // members
    by_first = (((0,), (0,)), ((), ()))
    for c in range(cells):
        field = field_ref[pl.ds(c, members, stride=cells), :]
        anomaly = field - jnp.sum(field, axis=0, keepdims=True) / members
        moved = lax.dot_general(weights, anomaly, by_first, precision=HIGHEST, preferred_element_type=jnp.float32)
        out_ref[pl.ds(c, members, stride=cells), :] = field + moved
    predicted.wait()


def exchange(x):
    return lax.all_to_all(x, AXES, split_axis=0, concat_axis=0, tiled=True)


def local_whole(ensemble, source, obs_rows, obs_values, obs_noise, obs_var):
    members = ensemble.shape[0]
    bx, by, nz = source.shape
    n_m, n_s = lax.axis_size("member"), lax.axis_size("space")
    devices = n_m * n_s
    held = members // devices
    block = bx * by
    n_obs = obs_rows.shape[-1]
    rows = (held + 1) * block + n_obs
    packed = vmem_call(
        pack_kernel,
        pltpu.VMEM((devices, rows, 1, nz), jnp.float32),
        [
            pltpu.VMEM((block, 1, nz), jnp.float32),
            pltpu.SMEM((n_obs,), jnp.int32),
            pltpu.SemaphoreType.DMA((3,)),
        ],
        "pack",
        ensemble.reshape(devices, held * block, 1, nz),
        source.reshape(block, 1, nz),
        obs_rows.reshape(-1),
        spaces=[pl.ANY] * 3,
    )
    got = exchange(packed.reshape(devices * rows, 1, nz)).reshape(devices * rows, nz)
    nx, ny = n_s * bx, n_m * by
    field = pltpu.VMEM((held * nx * ny + 2 * TILE, nz), jnp.float32)
    plane = pltpu.VMEM((held * ny, nz), jnp.float32)
    observed = n_obs * nz
    row = pltpu.VMEM((1, observed), jnp.float32)
    picked, aim, scale = vmem_call(
        functools.partial(pressure_kernel, dims=(n_m, n_s, held, bx, by, n_obs)),
        [pltpu.VMEM((members * n_obs, nz), jnp.float32), pltpu.VMEM((members, observed), jnp.float32), row],
        [row] * 2 + [pltpu.SemaphoreType.DMA((3,))] + [field] * 9 + [plane] * 2,
        "pressure",
        near(got),
        obs_values.reshape(1, observed),
        obs_noise.reshape(members, observed),
        obs_var.reshape(1, observed),
        spaces=[pltpu.VMEM] + [pl.ANY] * 3,
        outs=[pl.BlockSpec(memory_space=pltpu.VMEM)] * 3,
    )
    returned = exchange(picked.reshape(members * n_obs, 1, nz))
    sums = vmem_call(
        functools.partial(sums_kernel, devices=devices),
        pltpu.VMEM((devices, 2 * held, members), jnp.float32),
        [],
        "sums",
        near(returned.reshape(members, observed)),
        near(aim),
        near(scale),
    )
    own = vmem_call(spread_kernel, pltpu.VMEM(sums.shape, jnp.float32), [], "spread", near(exchange(sums)))
    gathered = exchange(own)
    updated, predicted = vmem_call(
        functools.partial(update_kernel, devices=devices),
        [
            jax.ShapeDtypeStruct((members * block, nz), jnp.float32),
            jax.ShapeDtypeStruct((members, n_obs * nz), jnp.float32),
        ],
        [pltpu.VMEM((members, members), jnp.float32)] * 2 + [pltpu.SemaphoreType.DMA],
        "update",
        near(gathered),
        near(ensemble.reshape(members * block, nz)),
        near(returned.reshape(members, n_obs * nz)),
        outs=[pl.BlockSpec(memory_space=pltpu.VMEM), pl.BlockSpec(memory_space=pl.ANY)],
    )
    return (updated.reshape(ensemble.shape), predicted.reshape(members, 1, 1, n_obs * nz))


def local(ensemble, *rest):
    devices = lax.axis_size("member") * lax.axis_size("space")
    form = local_whole if ensemble.shape[0] % devices == 0 else local_split
    return form(ensemble, *rest)


def solution(mesh):
    in_specs = (
        P(None, "space", "member", None),
        P("space", "member", None),
        P("space", "member", None),
        P("space", "member", None),
        P(None, "space", "member", None),
        P("space", "member", None),
    )
    out_specs = (P(None, "space", "member", None), P(None, "space", "member", None))
    return jax.shard_map(local, mesh=mesh, in_specs=in_specs, out_specs=out_specs, check_vma=False)
```

```python
import functools

import jax
import jax.numpy as jnp
from jax import lax
from jax.experimental import pallas as pl
from jax.experimental.pallas import tpu as pltpu
from jax.sharding import PartitionSpec as P

ITERS = 4
TILE = 8
AXES = ("member", "space")
HIGHEST = lax.Precision.HIGHEST


def padded_2(x, sides, width):
    for axis, dim in sides:
        devices, length = (lax.axis_size(axis), x.shape[dim])
        up = [(i, (i + 1) % devices) for i in range(devices - 1)]
        down = [(j, i) for i, j in up]
        last = lax.slice_in_dim(x, length - width, length, axis=dim)
        leading = lax.slice_in_dim(x, 0, width, axis=dim)
        before = lax.ppermute(last, axis, up)
        after = lax.ppermute(leading, axis, down)
        x = jnp.concatenate([before, x, after], axis=dim)
    return x


def harmonic(first_cond, second_cond):
    return 2.0 * first_cond * second_cond / (first_cond + second_cond)


def extend(values_in):
    widened = padded_2(values_in, (("member", 2),), 1)
    return jnp.pad(widened, ((0, 0), (1, 1), (0, 0), (1, 1)))


def member_dots(dot_terms):
    return lax.psum(dot_terms, "member")


def face_terms(cond):
    widened = extend(cond)
    edge_pad = jnp.pad(cond, ((0, 0), (1, 1), (1, 1), (1, 1)), mode="edge")
    cond_pad = jnp.where(widened > 0.0, widened, edge_pad)
    face_x = harmonic(cond_pad[:, :-1, 1:-1, 1:-1], cond_pad[:, 1:, 1:-1, 1:-1])
    face_y = harmonic(cond_pad[:, 1:-1, :-1, 1:-1], cond_pad[:, 1:-1, 1:, 1:-1])
    face_z = harmonic(cond, cond_pad[:, 1:-1, 1:-1, 2:])
    lower_z = jnp.concatenate([harmonic(cond[..., :1], cond[..., :1]), face_z[..., :-1]], axis=-1)
    return (face_x, face_y, face_z, lower_z)


def operate(values_in, face_x, face_y, face_z, lower_z):
    padded = extend(values_in)
    result = face_x[:, 1:] * (values_in - padded[:, 2:, 1:-1, 1:-1]) + face_x[:, :-1] * (
        values_in - padded[:, :-2, 1:-1, 1:-1]
    )
    result = (
        result
        + face_y[:, :, 1:] * (values_in - padded[:, 1:-1, 2:, 1:-1])
        + face_y[:, :, :-1] * (values_in - padded[:, 1:-1, :-2, 1:-1])
    )
    result = (
        result
        + face_z * (values_in - padded[:, 1:-1, 1:-1, 2:])
        + lower_z * (values_in - padded[:, 1:-1, 1:-1, :-2])
    )
    return result


def conjugate(cond, forcing):
    face_x, face_y, face_z, lower_z = face_terms(cond)
    residual = jnp.broadcast_to(forcing[None], cond.shape)
    direction = residual
    solution = jnp.zeros_like(cond)
    norm_now = member_dots(jnp.sum(residual * residual, axis=(1, 2, 3)))
    for iteration in range(ITERS):
        image = operate(direction, face_x, face_y, face_z, lower_z)
        step_size = norm_now / member_dots(jnp.sum(direction * image, axis=(1, 2, 3)))
        solution = solution + step_size[:, None, None, None] * direction
        residual = residual - step_size[:, None, None, None] * image
        if iteration + 1 < ITERS:
            norm_next = member_dots(jnp.sum(residual * residual, axis=(1, 2, 3)))
            direction = residual + (norm_next / norm_now)[:, None, None, None] * direction
            norm_now = norm_next
    return solution


def local_split(ensemble, source, obs_rows, obs_values, obs_noise, obs_var):
    total_members = ensemble.shape[0]
    block_x, block_y, layers = source.shape
    held_fields = lax.all_to_all(ensemble, "space", split_axis=0, concat_axis=1, tiled=True)
    forcing = lax.all_gather(source, "space", axis=0, tiled=True)
    pressure = conjugate(jnp.exp(held_fields), forcing)
    held_count = pressure.shape[0]
    cells_flat = pressure.reshape(held_count, -1, layers)
    gathered_rows = lax.all_gather(obs_rows, "space", axis=0, tiled=True)
    row_ids = gathered_rows[:, 0]
    peer_ids = jnp.arange(row_ids.shape[0], dtype=jnp.int32)[:, None]
    flat_index = (peer_ids * block_x + row_ids // block_y) * block_y + row_ids % block_y
    picked = jnp.take(cells_flat, flat_index.reshape(-1), axis=1)
    returned = lax.all_to_all(picked, "space", split_axis=1, concat_axis=0, tiled=True)
    predicted = returned.reshape(total_members, 1, 1, -1)
    flat_pred = returned.reshape(total_members, -1)
    inv_sigma = 1.0 / jnp.sqrt(obs_var.reshape(-1))
    spread = (flat_pred - jnp.mean(flat_pred, axis=0)) * inv_sigma
    misfit = (obs_values.reshape(-1) - flat_pred) * inv_sigma + obs_noise.reshape(total_members, -1)
    gram_part = jnp.dot(spread, spread.T, precision=HIGHEST)
    cross_part = jnp.dot(spread, misfit.T, precision=HIGHEST)
    gram_sum, cross_sum = lax.psum((gram_part, cross_part), AXES)
    factor = jnp.linalg.cholesky(
        gram_sum + (total_members - 1.0) * jnp.eye(total_members, dtype=jnp.float32)
    )
    weights = jax.scipy.linalg.cho_solve((factor, True), cross_sum)
    flat_field = ensemble.reshape(total_members, -1)
    anomalies = flat_field - jnp.mean(flat_field, axis=0)
    updated = flat_field + jnp.dot(weights.T, anomalies, precision=HIGHEST)
    return (updated.reshape(ensemble.shape), predicted)


def vmem_call(kernel, out, scratch, name, *operands, spaces=None, outs=pl.BlockSpec(memory_space=pltpu.VMEM)):
    specs = [pl.BlockSpec(memory_space=s) for s in spaces or [pltpu.VMEM] * len(operands)]
    return pl.pallas_call(
        kernel,
        out_shape=out,
        in_specs=specs,
        out_specs=outs,
        scratch_shapes=scratch,
        name=name,
    )(*operands)


def near(x):
    return pltpu.with_memory_space_constraint(x, pltpu.VMEM)


def pack_kernel(field_ref, source_ref, obs_ref, out_ref, block_ref, rows_ref, sems):
    devices, _, _, nz = out_ref.shape
    cells, block, n_obs = field_ref.shape[1], source_ref.shape[0], obs_ref.shape[0]
    fields = pltpu.make_async_copy(field_ref, out_ref.at[:, pl.ds(0, cells)], sems.at[0])
    source = pltpu.make_async_copy(source_ref, block_ref, sems.at[1])
    rows = pltpu.make_async_copy(obs_ref, rows_ref, sems.at[2])
    rows.start()
    source.start()
    fields.start()
    rows.wait()
    for o in range(n_obs):
        pick = jnp.full((1, 1, nz), rows_ref[o].astype(jnp.float32))
        for d in range(devices):
            out_ref[d, pl.ds(cells + block + o, 1)] = pick
    source.wait()
    held = block_ref[...]
    for d in range(devices):
        out_ref[d, pl.ds(cells, block)] = held
    fields.wait()


def total(acc):
    return jnp.sum(jnp.sum(acc, axis=0, keepdims=True), axis=1, keepdims=True)


def pressure_kernel(g_ref, values_hbm, noise_hbm, var_hbm, out_ref, aim_ref, scale_ref, values_ref, var_ref, sems, e_ref, fx_ref, fy_ref, fz_ref, mid_ref, p_ref, r_ref, q_ref, x_ref, acc_ref, norm_ref, *, dims):
    n_m, n_s, held, bx, by, n_obs = dims
    nx, ny = n_s * bx, n_m * by
    nz = g_ref.shape[1]
    block = bx * by
    rows = (held + 1) * block + n_obs
    plane = (ny, nz)
    fetched = ((noise_hbm, aim_ref), (values_hbm, values_ref), (var_hbm, var_ref))
    fetches = [pltpu.make_async_copy(x, y, sems.at[i]) for i, (x, y) in enumerate(fetched)]
    for fetch in fetches:
        fetch.start()
    lane = lax.broadcasted_iota(jnp.int32, plane, 1)
    sub = lax.broadcasted_iota(jnp.int32, plane, 0)

    def at(j, x, shift=0):
        start = pl.multiple_of((j * nx + x) * ny, ny)
        return pl.ds(start + (TILE + shift), ny)

    def member(j):
        return pl.ds(pl.multiple_of(j * ny, ny), ny)

    def for_members(fn):
        def body(j, carry):
            fn(j)
            return carry

        lax.fori_loop(0, held, body, 0, unroll=2 - held % 2)

    for ref in (p_ref, fy_ref):
        for edge in (0, TILE + held * nx * ny):
            ref[pl.ds(edge, TILE), :] = jnp.zeros((TILE, nz), jnp.float32)

    for m in range(n_m):
        for s in range(n_s):
            base = (m * n_s + s) * rows
            for a in range(bx):
                x = s * bx + a
                for j in range(held):
                    e_ref[pl.ds(TILE + (j * nx + x) * ny + m * by, by), :] = g_ref[
                        pl.ds(base + j * block + a * by, by), :
                    ]
                x_ref[pl.ds(TILE + x * ny + m * by, by), :] = g_ref[pl.ds(base + held * block + a * by, by), :]

    norm0 = jnp.zeros(plane, jnp.float32)
    for x in range(nx):
        v = x_ref[at(0, x), :]
        norm0 = norm0 + v * v
        for j in range(held):
            p_ref[at(j, x), :] = v
            r_ref[at(j, x), :] = v
    norm0 = jnp.broadcast_to(total(norm0), plane)
    for j in range(held):
        norm_ref[member(j), :] = norm0
    x_ref[...] = jnp.zeros(x_ref.shape, jnp.float32)

    edge_z = (lane == 0).astype(jnp.float32) + (lane == nz - 1).astype(jnp.float32)
    edge_y = (sub == 0).astype(jnp.float32) + (sub == ny - 1).astype(jnp.float32)

    def faces(j):
        e = jnp.exp(-e_ref[at(j, 0), :])
        fx = None
        for x in range(nx):
            fy = jnp.where(sub > 0, 2.0 / (e + pltpu.roll(e, 1, 0)), 0.0)
            fz = jnp.where(lane > 0, 2.0 / (e + pltpu.roll(e, 1, 1)), 0.0)
            fy_ref[at(j, x), :] = fy
            fz_ref[at(j, x), :] = fz
            fz_up = jnp.where(lane < nz - 1, 2.0 / (e + pltpu.roll(e, nz - 1, 1)), 0.0)
            mid = (fy + pltpu.roll(fy, ny - 1, 0)) + (fz + fz_up)
            ends = edge_y + edge_z
            if x == 0 or x == nx - 1:
                ends = ends + 1.0
            mid = mid + ends / e
            if fx is not None:
                mid = mid + fx
            if x + 1 < nx:
                after = jnp.exp(-e_ref[at(j, x + 1), :])
                fx = 2.0 / (e + after)
                fx_ref[at(j, x + 1), :] = fx
                mid = mid + fx
                e = after
            mid_ref[at(j, x), :] = mid

    for_members(faces)

    def turn(j, ratio):
        for x in range(nx):
            v = r_ref[at(j, x), :] + ratio * p_ref[at(j, x), :]
            p_ref[at(j, x), :] = v
            f = fz_ref[at(j, x), :]
            q_ref[at(j, x), :] = f * pltpu.roll(v, 1, 1) + pltpu.roll(f * v, nz - 1, 1)
            yield

    def apply(j, dots):
        acc = jnp.zeros(plane, jnp.float32)
        before, fx = None, None
        v = p_ref[at(j, 0), :]
        for x in range(nx):
            image = mid_ref[at(j, x), :] * v - q_ref[at(j, x), :]
            image = image - fy_ref[at(j, x), :] * p_ref[at(j, x, -1), :]
            image = image - fy_ref[at(j, x, 1), :] * p_ref[at(j, x, 1), :]
            if x > 0:
                image = image - fx * before
            if x + 1 < nx:
                after = p_ref[at(j, x + 1), :]
                fx = fx_ref[at(j, x + 1), :]
                image = image - fx * after
            q_ref[at(j, x), :] = image
            acc = acc + v * image
            if x + 1 < nx:
                before, v = v, after
            yield
        dots[j] = acc

    def move(j, step, norms):
        acc = jnp.zeros(plane, jnp.float32)
        for x in range(nx):
            x_ref[at(j, x), :] = x_ref[at(j, x), :] + step * p_ref[at(j, x), :]
            res = r_ref[at(j, x), :] - step * q_ref[at(j, x), :]
            r_ref[at(j, x), :] = res
            acc = acc + res * res
            yield
        norms[j] = acc

    def together(*stages):
        stages = list(stages)
        while stages:
            stages = [stage for stage in stages if next(stage, stage) is not stage]

    def spread_total(acc):
        return jnp.broadcast_to(total(acc), plane)

    def steps_of(dots):
        return {j: norm_ref[member(j), :] / spread_total(dot) for j, dot in dots.items()}

    def ratios_of(norms):
        ratios = {}
        for j, norm in norms.items():
            norm = spread_total(norm)
            ratios[j] = norm / norm_ref[member(j), :]
            norm_ref[member(j), :] = norm
        return ratios

    ahead, behind = range(held // 2), range(held // 2, held)

    def open_stage():
        dots = {}
        together(*[apply(j, dots) for j in ahead], *[turn(j, acc_ref[member(j), :]) for j in behind])
        return steps_of(dots)

    def one(iteration, carry):
        steps, dots, norms = open_stage(), {}, {}
        together(*[apply(j, dots) for j in behind], *[move(j, steps[j], norms) for j in ahead])
        ratios, steps, norms = ratios_of(norms), steps_of(dots), {}
        together(*[turn(j, ratios[j]) for j in ahead], *[move(j, steps[j], norms) for j in behind])
        for j, ratio in ratios_of(norms).items():
            acc_ref[member(j), :] = ratio
        return carry

    acc_ref[...] = jnp.zeros(acc_ref.shape, jnp.float32)
    together(*[turn(j, acc_ref[member(j), :]) for j in ahead])
    lax.fori_loop(0, ITERS - 1, one, 0)
    steps, dots = open_stage(), {}
    together(*[apply(j, dots) for j in behind])
    steps.update(steps_of(dots))
    for j, step in steps.items():
        acc_ref[member(j), :] = step

    for fetch in fetches:
        fetch.wait()
    inv_sigma = 1.0 / jnp.sqrt(var_ref[...])
    scale_ref[...] = inv_sigma
    aim_ref[...] = aim_ref[...] + values_ref[...] * inv_sigma

    for m in range(n_m):
        for s in range(n_s):
            peer = m * n_s + s
            for o in range(n_obs):
                picked = g_ref[pl.ds(peer * rows + (held + 1) * block + o, 1), :].astype(jnp.int32)[0, 0]
                cell = (s * bx + picked // by) * ny + m * by + picked % by
                for j in range(held):
                    row = pl.ds(TILE + j * nx * ny + cell, 1)
                    out_ref[pl.ds((peer * held + j) * n_obs + o, 1), :] = (
                        x_ref[row, :] + acc_ref[pl.ds(j * ny, 1), :] * p_ref[row, :]
                    )


def sums_kernel(pred_ref, aim_ref, scale_ref, out_ref, *, devices):
    members = pred_ref.shape[0]
    held = members // devices
    pred = pred_ref[...]
    inv_sigma = scale_ref[...]
    mean = jnp.sum(pred, axis=0, keepdims=True) / members
    spread = (pred - mean) * inv_sigma
    misfit = aim_ref[...] - pred * inv_sigma
    by_last = (((1,), (1,)), ((), ()))
    gram = lax.dot_general(spread, spread, by_last, precision=HIGHEST, preferred_element_type=jnp.float32)
    cross = lax.dot_general(spread, misfit, by_last, precision=HIGHEST, preferred_element_type=jnp.float32)
    for d in range(devices):
        out_ref[d, 0:held, :] = gram[d * held : (d + 1) * held, :]
        out_ref[d, held : 2 * held, :] = cross[d * held : (d + 1) * held, :]


def spread_kernel(parts_ref, out_ref):
    devices = parts_ref.shape[0]
    own = jnp.sum(parts_ref[...], axis=0)
    for d in range(devices):
        out_ref[d] = own


def update_kernel(sums_ref, field_ref, found_ref, out_ref, predicted_ref, a_ref, c_ref, sem, *, devices):
    predicted = pltpu.make_async_copy(found_ref, predicted_ref, sem)
    predicted.start()
    members = sums_ref.shape[2]
    held = members // devices
    tile = 8
    for d in range(devices):
        a_ref[pl.ds(d * held, held), :] = sums_ref[d, 0:held, :]
        c_ref[pl.ds(d * held, held), :] = sums_ref[d, held : 2 * held, :]
    lane = lax.broadcasted_iota(jnp.int32, (tile, members), 1)
    sub = lax.broadcasted_iota(jnp.int32, (tile, members), 0)
    blocks = members // tile
    ones = (lane >= 0).astype(jnp.float32)
    left, right = [], []
    for k in range(blocks):
        own = (lane == sub + k * tile).astype(jnp.float32) * (members - 1.0)
        left.append(a_ref[pl.ds(k * tile, tile), :] + own)
        right.append(c_ref[pl.ds(k * tile, tile), :])
    wide = (tile, members)

    def row(x, t):
        return jnp.broadcast_to(x[t : t + 1, :], wide)

    def column(x, t):
        return jnp.broadcast_to(x[:, t : t + 1], wide)

    for k in range(blocks):
        parts = [column(left[k], k * tile + t) * ones for t in range(tile)] + [left[k], right[k]]
        for t in range(tile):
            inverse = 1.0 / row(parts[t], t)
            factor = jnp.where(sub == t, 0.0, parts[t] * inverse)
            scaled = sub == t
            for i in range(t + 1, len(parts)):
                pivot = row(parts[i], t)
                parts[i] = jnp.where(scaled, pivot * inverse, parts[i] - factor * pivot)
        left[k], right[k] = parts[-2], parts[-1]
        rows_left = [row(left[k], t) for t in range(tile)]
        rows_right = [row(right[k], t) for t in range(tile)]
        for i in range(blocks):
            if i != k:
                columns = [column(left[i], k * tile + t) for t in range(tile)]
                for t in range(tile):
                    right[i] = right[i] - columns[t] * rows_right[t]
                    if k + 1 < blocks:
                        left[i] = left[i] - columns[t] * rows_left[t]
    for k in range(blocks):
        c_ref[pl.ds(k * tile, tile), :] = right[k]
    weights = c_ref[...]
    cells = field_ref.shape[0] // members
    by_first = (((0,), (0,)), ((), ()))
    for c in range(cells):
        field = field_ref[pl.ds(c, members, stride=cells), :]
        anomaly = field - jnp.sum(field, axis=0, keepdims=True) / members
        moved = lax.dot_general(weights, anomaly, by_first, precision=HIGHEST, preferred_element_type=jnp.float32)
        out_ref[pl.ds(c, members, stride=cells), :] = field + moved
    predicted.wait()


def exchange(x):
    return lax.all_to_all(x, AXES, split_axis=0, concat_axis=0, tiled=True)


def local_whole(ensemble, source, obs_rows, obs_values, obs_noise, obs_var):
    members = ensemble.shape[0]
    bx, by, nz = source.shape
    n_m, n_s = lax.axis_size("member"), lax.axis_size("space")
    devices = n_m * n_s
    held = members // devices
    block = bx * by
    n_obs = obs_rows.shape[-1]
    rows = (held + 1) * block + n_obs
    packed = vmem_call(
        pack_kernel,
        pltpu.VMEM((devices, rows, 1, nz), jnp.float32),
        [
            pltpu.VMEM((block, 1, nz), jnp.float32),
            pltpu.SMEM((n_obs,), jnp.int32),
            pltpu.SemaphoreType.DMA((3,)),
        ],
        "pack",
        ensemble.reshape(devices, held * block, 1, nz),
        source.reshape(block, 1, nz),
        obs_rows.reshape(-1),
        spaces=[pl.ANY] * 3,
    )
    got = exchange(packed.reshape(devices * rows, 1, nz)).reshape(devices * rows, nz)
    nx, ny = n_s * bx, n_m * by
    field = pltpu.VMEM((held * nx * ny + 2 * TILE, nz), jnp.float32)
    plane = pltpu.VMEM((held * ny, nz), jnp.float32)
    observed = n_obs * nz
    row = pltpu.VMEM((1, observed), jnp.float32)
    picked, aim, scale = vmem_call(
        functools.partial(pressure_kernel, dims=(n_m, n_s, held, bx, by, n_obs)),
        [pltpu.VMEM((members * n_obs, nz), jnp.float32), pltpu.VMEM((members, observed), jnp.float32), row],
        [row] * 2 + [pltpu.SemaphoreType.DMA((3,))] + [field] * 9 + [plane] * 2,
        "pressure",
        near(got),
        obs_values.reshape(1, observed),
        obs_noise.reshape(members, observed),
        obs_var.reshape(1, observed),
        spaces=[pltpu.VMEM] + [pl.ANY] * 3,
        outs=[pl.BlockSpec(memory_space=pltpu.VMEM)] * 3,
    )
    returned = exchange(picked.reshape(members * n_obs, 1, nz))
    sums = vmem_call(
        functools.partial(sums_kernel, devices=devices),
        pltpu.VMEM((devices, 2 * held, members), jnp.float32),
        [],
        "sums",
        near(returned.reshape(members, observed)),
        near(aim),
        near(scale),
    )
    own = vmem_call(spread_kernel, pltpu.VMEM(sums.shape, jnp.float32), [], "spread", near(exchange(sums)))
    gathered = exchange(own)
    updated, predicted = vmem_call(
        functools.partial(update_kernel, devices=devices),
        [
            jax.ShapeDtypeStruct((members * block, nz), jnp.float32),
            jax.ShapeDtypeStruct((members, n_obs * nz), jnp.float32),
        ],
        [pltpu.VMEM((members, members), jnp.float32)] * 2 + [pltpu.SemaphoreType.DMA],
        "update",
        near(gathered),
        near(ensemble.reshape(members * block, nz)),
        near(returned.reshape(members, n_obs * nz)),
        outs=[pl.BlockSpec(memory_space=pltpu.VMEM), pl.BlockSpec(memory_space=pl.ANY)],
    )
    return (updated.reshape(ensemble.shape), predicted.reshape(members, 1, 1, n_obs * nz))


def local(ensemble, *rest):
    devices = lax.axis_size("member") * lax.axis_size("space")
    form = local_whole if ensemble.shape[0] % devices == 0 else local_split
    return form(ensemble, *rest)


def solution(mesh):
    in_specs = (
        P(None, "space", "member", None),
        P("space", "member", None),
        P("space", "member", None),
        P("space", "member", None),
        P(None, "space", "member", None),
        P("space", "member", None),
    )
    out_specs = (P(None, "space", "member", None), P(None, "space", "member", None))
    return jax.shard_map(local, mesh=mesh, in_specs=in_specs, out_specs=out_specs, check_vma=False)
```

```python
import functools

import jax
import jax.numpy as jnp
from jax import lax
from jax.experimental import pallas as pl
from jax.experimental.pallas import tpu as pltpu
from jax.sharding import PartitionSpec as P

ITERS = 4
TILE = 8
AXES = ("member", "space")
HIGHEST = lax.Precision.HIGHEST


def padded_2(x, sides, width):
    for axis, dim in sides:
        devices, length = (lax.axis_size(axis), x.shape[dim])
        up = [(i, (i + 1) % devices) for i in range(devices - 1)]
        down = [(j, i) for i, j in up]
        last = lax.slice_in_dim(x, length - width, length, axis=dim)
        leading = lax.slice_in_dim(x, 0, width, axis=dim)
        before = lax.ppermute(last, axis, up)
        after = lax.ppermute(leading, axis, down)
        x = jnp.concatenate([before, x, after], axis=dim)
    return x


def harmonic(first_cond, second_cond):
    return 2.0 * first_cond * second_cond / (first_cond + second_cond)


def extend(values_in):
    widened = padded_2(values_in, (("member", 2),), 1)
    return jnp.pad(widened, ((0, 0), (1, 1), (0, 0), (1, 1)))


def member_dots(dot_terms):
    return lax.psum(dot_terms, "member")


def face_terms(cond):
    widened = extend(cond)
    edge_pad = jnp.pad(cond, ((0, 0), (1, 1), (1, 1), (1, 1)), mode="edge")
    cond_pad = jnp.where(widened > 0.0, widened, edge_pad)
    face_x = harmonic(cond_pad[:, :-1, 1:-1, 1:-1], cond_pad[:, 1:, 1:-1, 1:-1])
    face_y = harmonic(cond_pad[:, 1:-1, :-1, 1:-1], cond_pad[:, 1:-1, 1:, 1:-1])
    face_z = harmonic(cond, cond_pad[:, 1:-1, 1:-1, 2:])
    lower_z = jnp.concatenate([harmonic(cond[..., :1], cond[..., :1]), face_z[..., :-1]], axis=-1)
    return (face_x, face_y, face_z, lower_z)


def operate(values_in, face_x, face_y, face_z, lower_z):
    padded = extend(values_in)
    result = face_x[:, 1:] * (values_in - padded[:, 2:, 1:-1, 1:-1]) + face_x[:, :-1] * (
        values_in - padded[:, :-2, 1:-1, 1:-1]
    )
    result = (
        result
        + face_y[:, :, 1:] * (values_in - padded[:, 1:-1, 2:, 1:-1])
        + face_y[:, :, :-1] * (values_in - padded[:, 1:-1, :-2, 1:-1])
    )
    result = (
        result
        + face_z * (values_in - padded[:, 1:-1, 1:-1, 2:])
        + lower_z * (values_in - padded[:, 1:-1, 1:-1, :-2])
    )
    return result


def conjugate(cond, forcing):
    face_x, face_y, face_z, lower_z = face_terms(cond)
    residual = jnp.broadcast_to(forcing[None], cond.shape)
    direction = residual
    solution = jnp.zeros_like(cond)
    norm_now = member_dots(jnp.sum(residual * residual, axis=(1, 2, 3)))
    for iteration in range(ITERS):
        image = operate(direction, face_x, face_y, face_z, lower_z)
        step_size = norm_now / member_dots(jnp.sum(direction * image, axis=(1, 2, 3)))
        solution = solution + step_size[:, None, None, None] * direction
        residual = residual - step_size[:, None, None, None] * image
        if iteration + 1 < ITERS:
            norm_next = member_dots(jnp.sum(residual * residual, axis=(1, 2, 3)))
            direction = residual + (norm_next / norm_now)[:, None, None, None] * direction
            norm_now = norm_next
    return solution


def local_split(ensemble, source, obs_rows, obs_values, obs_noise, obs_var):
    total_members = ensemble.shape[0]
    block_x, block_y, layers = source.shape
    held_fields = lax.all_to_all(ensemble, "space", split_axis=0, concat_axis=1, tiled=True)
    forcing = lax.all_gather(source, "space", axis=0, tiled=True)
    pressure = conjugate(jnp.exp(held_fields), forcing)
    held_count = pressure.shape[0]
    cells_flat = pressure.reshape(held_count, -1, layers)
    gathered_rows = lax.all_gather(obs_rows, "space", axis=0, tiled=True)
    row_ids = gathered_rows[:, 0]
    peer_ids = jnp.arange(row_ids.shape[0], dtype=jnp.int32)[:, None]
    flat_index = (peer_ids * block_x + row_ids // block_y) * block_y + row_ids % block_y
    picked = jnp.take(cells_flat, flat_index.reshape(-1), axis=1)
    returned = lax.all_to_all(picked, "space", split_axis=1, concat_axis=0, tiled=True)
    predicted = returned.reshape(total_members, 1, 1, -1)
    flat_pred = returned.reshape(total_members, -1)
    inv_sigma = 1.0 / jnp.sqrt(obs_var.reshape(-1))
    spread = (flat_pred - jnp.mean(flat_pred, axis=0)) * inv_sigma
    misfit = (obs_values.reshape(-1) - flat_pred) * inv_sigma + obs_noise.reshape(total_members, -1)
    gram_part = jnp.dot(spread, spread.T, precision=HIGHEST)
    cross_part = jnp.dot(spread, misfit.T, precision=HIGHEST)
    gram_sum, cross_sum = lax.psum((gram_part, cross_part), AXES)
    factor = jnp.linalg.cholesky(
        gram_sum + (total_members - 1.0) * jnp.eye(total_members, dtype=jnp.float32)
    )
    weights = jax.scipy.linalg.cho_solve((factor, True), cross_sum)
    flat_field = ensemble.reshape(total_members, -1)
    anomalies = flat_field - jnp.mean(flat_field, axis=0)
    updated = flat_field + jnp.dot(weights.T, anomalies, precision=HIGHEST)
    return (updated.reshape(ensemble.shape), predicted)


def vmem_call(kernel, out, scratch, name, *operands, spaces=None, outs=pl.BlockSpec(memory_space=pltpu.VMEM)):
    specs = [pl.BlockSpec(memory_space=s) for s in spaces or [pltpu.VMEM] * len(operands)]
    return pl.pallas_call(
        kernel,
        out_shape=out,
        in_specs=specs,
        out_specs=outs,
        scratch_shapes=scratch,
        name=name,
    )(*operands)


def near(x):
    return pltpu.with_memory_space_constraint(x, pltpu.VMEM)


def pack_kernel(field_ref, source_ref, obs_ref, out_ref, block_ref, rows_ref, sems):
    devices, _, _, nz = out_ref.shape
    cells, block, n_obs = field_ref.shape[1], source_ref.shape[0], obs_ref.shape[0]
    fields = pltpu.make_async_copy(field_ref, out_ref.at[:, pl.ds(0, cells)], sems.at[0])
    source = pltpu.make_async_copy(source_ref, block_ref, sems.at[1])
    rows = pltpu.make_async_copy(obs_ref, rows_ref, sems.at[2])
    fields.start()
    rows.start()
    source.start()
    rows.wait()
    for o in range(n_obs):
        pick = jnp.full((1, 1, nz), rows_ref[o].astype(jnp.float32))
        for d in range(devices):
            out_ref[d, pl.ds(cells + block + o, 1)] = pick
    source.wait()
    held = block_ref[...]
    for d in range(devices):
        out_ref[d, pl.ds(cells, block)] = held
    fields.wait()


def total(acc):
    return jnp.sum(jnp.sum(acc, axis=0, keepdims=True), axis=1, keepdims=True)


def pressure_kernel(g_ref, values_hbm, noise_hbm, var_hbm, out_ref, aim_ref, scale_ref, values_ref, var_ref, sems, e_ref, fx_ref, fy_ref, fz_ref, mid_ref, p_ref, r_ref, q_ref, x_ref, acc_ref, norm_ref, *, dims):
    n_m, n_s, held, bx, by, n_obs = dims
    nx, ny = n_s * bx, n_m * by
    nz = g_ref.shape[1]
    block = bx * by
    rows = (held + 1) * block + n_obs
    plane = (ny, nz)
    fetched = ((noise_hbm, aim_ref), (values_hbm, values_ref), (var_hbm, var_ref))
    fetches = [pltpu.make_async_copy(x, y, sems.at[i]) for i, (x, y) in enumerate(fetched)]
    for fetch in fetches:
        fetch.start()
    lane = lax.broadcasted_iota(jnp.int32, plane, 1)
    sub = lax.broadcasted_iota(jnp.int32, plane, 0)

    def at(j, x, shift=0):
        start = pl.multiple_of((j * nx + x) * ny, ny)
        return pl.ds(start + (TILE + shift), ny)

    def member(j):
        return pl.ds(pl.multiple_of(j * ny, ny), ny)

    def for_members(fn):
        def body(j, carry):
            fn(j)
            return carry

        lax.fori_loop(0, held, body, 0, unroll=2 - held % 2)

    for ref in (p_ref, fy_ref):
        for edge in (0, TILE + held * nx * ny):
            ref[pl.ds(edge, TILE), :] = jnp.zeros((TILE, nz), jnp.float32)

    for m in range(n_m):
        for s in range(n_s):
            base = (m * n_s + s) * rows
            for a in range(bx):
                x = s * bx + a
                for j in range(held):
                    e_ref[pl.ds(TILE + (j * nx + x) * ny + m * by, by), :] = g_ref[
                        pl.ds(base + j * block + a * by, by), :
                    ]
                x_ref[pl.ds(TILE + x * ny + m * by, by), :] = g_ref[pl.ds(base + held * block + a * by, by), :]

    norm0 = jnp.zeros(plane, jnp.float32)
    for x in range(nx):
        v = x_ref[at(0, x), :]
        norm0 = norm0 + v * v
        for j in range(held):
            p_ref[at(j, x), :] = v
            r_ref[at(j, x), :] = v
    norm0 = jnp.broadcast_to(total(norm0), plane)
    for j in range(held):
        norm_ref[member(j), :] = norm0
    x_ref[...] = jnp.zeros(x_ref.shape, jnp.float32)

    edge_z = (lane == 0).astype(jnp.float32) + (lane == nz - 1).astype(jnp.float32)
    edge_y = (sub == 0).astype(jnp.float32) + (sub == ny - 1).astype(jnp.float32)

    def faces(j):
        e = jnp.exp(-e_ref[at(j, 0), :])
        fx = None
        for x in range(nx):
            fy = jnp.where(sub > 0, 2.0 / (e + pltpu.roll(e, 1, 0)), 0.0)
            fz = jnp.where(lane > 0, 2.0 / (e + pltpu.roll(e, 1, 1)), 0.0)
            fy_ref[at(j, x), :] = fy
            fz_ref[at(j, x), :] = fz
            fz_up = jnp.where(lane < nz - 1, 2.0 / (e + pltpu.roll(e, nz - 1, 1)), 0.0)
            mid = (fy + pltpu.roll(fy, ny - 1, 0)) + (fz + fz_up)
            ends = edge_y + edge_z
            if x == 0 or x == nx - 1:
                ends = ends + 1.0
            mid = mid + ends / e
            if fx is not None:
                mid = mid + fx
            if x + 1 < nx:
                after = jnp.exp(-e_ref[at(j, x + 1), :])
                fx = 2.0 / (e + after)
                fx_ref[at(j, x + 1), :] = fx
                mid = mid + fx
                e = after
            mid_ref[at(j, x), :] = mid

    for_members(faces)

    def turn(j, ratio):
        for x in range(nx):
            v = r_ref[at(j, x), :]
            if ratio is not None:
                v = v + ratio * p_ref[at(j, x), :]
            p_ref[at(j, x), :] = v
            f = fz_ref[at(j, x), :]
            q_ref[at(j, x), :] = f * pltpu.roll(v, 1, 1) + pltpu.roll(f * v, nz - 1, 1)
            yield

    def apply(j, dots):
        acc = jnp.zeros(plane, jnp.float32)
        before, fx = None, None
        v = p_ref[at(j, 0), :]
        for x in range(nx):
            image = mid_ref[at(j, x), :] * v - q_ref[at(j, x), :]
            image = image - fy_ref[at(j, x), :] * p_ref[at(j, x, -1), :]
            image = image - fy_ref[at(j, x, 1), :] * p_ref[at(j, x, 1), :]
            if x > 0:
                image = image - fx * before
            if x + 1 < nx:
                after = p_ref[at(j, x + 1), :]
                fx = fx_ref[at(j, x + 1), :]
                image = image - fx * after
            q_ref[at(j, x), :] = image
            acc = acc + v * image
            if x + 1 < nx:
                before, v = v, after
            yield
        dots[j] = acc

    def move(j, step, norms):
        acc = jnp.zeros(plane, jnp.float32)
        for x in range(nx):
            x_ref[at(j, x), :] = x_ref[at(j, x), :] + step * p_ref[at(j, x), :]
            res = r_ref[at(j, x), :] - step * q_ref[at(j, x), :]
            r_ref[at(j, x), :] = res
            acc = acc + res * res
            yield
        norms[j] = acc

    def together(*stages):
        stages = list(stages)
        while stages:
            stages = [stage for stage in stages if next(stage, stage) is not stage]

    def spread_total(acc):
        return jnp.broadcast_to(total(acc), plane)

    def steps_of(dots):
        return {j: norm_ref[member(j), :] / spread_total(dot) for j, dot in dots.items()}

    def ratios_of(norms):
        ratios = {}
        for j, norm in norms.items():
            norm = spread_total(norm)
            ratios[j] = norm / norm_ref[member(j), :]
            norm_ref[member(j), :] = norm
        return ratios

    ahead, behind = range(held // 2), range(held // 2, held)

    def open_stage():
        dots = {}
        together(*[apply(j, dots) for j in ahead], *[turn(j, acc_ref[member(j), :]) for j in behind])
        return steps_of(dots)

    def one(iteration, carry):
        steps, dots, norms = open_stage(), {}, {}
        together(*[apply(j, dots) for j in behind], *[move(j, steps[j], norms) for j in ahead])
        ratios, steps, norms = ratios_of(norms), steps_of(dots), {}
        together(*[turn(j, ratios[j]) for j in ahead], *[move(j, steps[j], norms) for j in behind])
        for j, ratio in ratios_of(norms).items():
            acc_ref[member(j), :] = ratio
        return carry

    acc_ref[...] = jnp.zeros(acc_ref.shape, jnp.float32)
    together(*[turn(j, None) for j in ahead])
    lax.fori_loop(0, ITERS - 1, one, 0)
    steps, dots = open_stage(), {}
    together(*[apply(j, dots) for j in behind])
    steps.update(steps_of(dots))
    for j, step in steps.items():
        acc_ref[member(j), :] = step

    for fetch in fetches:
        fetch.wait()
    inv_sigma = 1.0 / jnp.sqrt(var_ref[...])
    scale_ref[...] = inv_sigma
    aim_ref[...] = aim_ref[...] + values_ref[...] * inv_sigma

    for m in range(n_m):
        for s in range(n_s):
            peer = m * n_s + s
            for o in range(n_obs):
                picked = g_ref[pl.ds(peer * rows + (held + 1) * block + o, 1), :].astype(jnp.int32)[0, 0]
                cell = (s * bx + picked // by) * ny + m * by + picked % by
                for j in range(held):
                    row = pl.ds(TILE + j * nx * ny + cell, 1)
                    out_ref[pl.ds((peer * held + j) * n_obs + o, 1), :] = (
                        x_ref[row, :] + acc_ref[pl.ds(j * ny, 1), :] * p_ref[row, :]
                    )


def sums_kernel(pred_ref, aim_ref, scale_ref, out_ref, *, devices):
    members = pred_ref.shape[0]
    held = members // devices
    pred = pred_ref[...]
    inv_sigma = scale_ref[...]
    mean = jnp.sum(pred, axis=0, keepdims=True) / members
    spread = (pred - mean) * inv_sigma
    misfit = aim_ref[...] - pred * inv_sigma
    by_last = (((1,), (1,)), ((), ()))
    gram = lax.dot_general(spread, spread, by_last, precision=HIGHEST, preferred_element_type=jnp.float32)
    cross = lax.dot_general(spread, misfit, by_last, precision=HIGHEST, preferred_element_type=jnp.float32)
    for d in range(devices):
        out_ref[d, 0:held, :] = gram[d * held : (d + 1) * held, :]
        out_ref[d, held : 2 * held, :] = cross[d * held : (d + 1) * held, :]


def spread_kernel(parts_ref, out_ref):
    devices = parts_ref.shape[0]
    own = jnp.sum(parts_ref[...], axis=0)
    for d in range(devices):
        out_ref[d] = own


def update_kernel(sums_ref, field_ref, found_ref, out_ref, predicted_ref, a_ref, c_ref, sem, *, devices):
    predicted = pltpu.make_async_copy(found_ref, predicted_ref, sem)
    predicted.start()
    members = sums_ref.shape[2]
    held = members // devices
    tile = 8
    for d in range(devices):
        a_ref[pl.ds(d * held, held), :] = sums_ref[d, 0:held, :]
        c_ref[pl.ds(d * held, held), :] = sums_ref[d, held : 2 * held, :]
    lane = lax.broadcasted_iota(jnp.int32, (tile, members), 1)
    sub = lax.broadcasted_iota(jnp.int32, (tile, members), 0)
    blocks = members // tile
    ones = (lane >= 0).astype(jnp.float32)
    left, right = [], []
    for k in range(blocks):
        own = (lane == sub + k * tile).astype(jnp.float32) * (members - 1.0)
        left.append(a_ref[pl.ds(k * tile, tile), :] + own)
        right.append(c_ref[pl.ds(k * tile, tile), :])
    wide = (tile, members)

    def row(x, t):
        return jnp.broadcast_to(x[t : t + 1, :], wide)

    def column(x, t):
        return jnp.broadcast_to(x[:, t : t + 1], wide)

    for k in range(blocks):
        parts = [column(left[k], k * tile + t) * ones for t in range(tile)] + [left[k], right[k]]
        for t in range(tile):
            inverse = 1.0 / row(parts[t], t)
            factor = jnp.where(sub == t, 0.0, parts[t] * inverse)
            scaled = sub == t
            for i in range(t + 1, len(parts)):
                pivot = row(parts[i], t)
                parts[i] = jnp.where(scaled, pivot * inverse, parts[i] - factor * pivot)
        left[k], right[k] = parts[-2], parts[-1]
        rows_left = [row(left[k], t) for t in range(tile)]
        rows_right = [row(right[k], t) for t in range(tile)]
        for i in range(blocks):
            if i != k:
                columns = [column(left[i], k * tile + t) for t in range(tile)]
                for t in range(tile):
                    right[i] = right[i] - columns[t] * rows_right[t]
                    if k + 1 < blocks:
                        left[i] = left[i] - columns[t] * rows_left[t]
    for k in range(blocks):
        c_ref[pl.ds(k * tile, tile), :] = right[k]
    weights = c_ref[...]
    cells = field_ref.shape[0] // members
    by_first = (((0,), (0,)), ((), ()))
    for c in range(cells):
        field = field_ref[pl.ds(c, members, stride=cells), :]
        anomaly = field - jnp.sum(field, axis=0, keepdims=True) / members
        moved = lax.dot_general(weights, anomaly, by_first, precision=HIGHEST, preferred_element_type=jnp.float32)
        out_ref[pl.ds(c, members, stride=cells), :] = field + moved
    predicted.wait()


def exchange(x):
    return lax.all_to_all(x, AXES, split_axis=0, concat_axis=0, tiled=True)


def local_whole(ensemble, source, obs_rows, obs_values, obs_noise, obs_var):
    members = ensemble.shape[0]
    bx, by, nz = source.shape
    n_m, n_s = lax.axis_size("member"), lax.axis_size("space")
    devices = n_m * n_s
    held = members // devices
    block = bx * by
    n_obs = obs_rows.shape[-1]
    rows = (held + 1) * block + n_obs
    packed = vmem_call(
        pack_kernel,
        pltpu.VMEM((devices, rows, 1, nz), jnp.float32),
        [
            pltpu.VMEM((block, 1, nz), jnp.float32),
            pltpu.SMEM((n_obs,), jnp.int32),
            pltpu.SemaphoreType.DMA((3,)),
        ],
        "pack",
        ensemble.reshape(devices, held * block, 1, nz),
        source.reshape(block, 1, nz),
        obs_rows.reshape(-1),
        spaces=[pl.ANY] * 3,
    )
    got = exchange(packed.reshape(devices * rows, 1, nz)).reshape(devices * rows, nz)
    nx, ny = n_s * bx, n_m * by
    field = pltpu.VMEM((held * nx * ny + 2 * TILE, nz), jnp.float32)
    plane = pltpu.VMEM((held * ny, nz), jnp.float32)
    observed = n_obs * nz
    row = pltpu.VMEM((1, observed), jnp.float32)
    picked, aim, scale = vmem_call(
        functools.partial(pressure_kernel, dims=(n_m, n_s, held, bx, by, n_obs)),
        [pltpu.VMEM((members * n_obs, nz), jnp.float32), pltpu.VMEM((members, observed), jnp.float32), row],
        [row] * 2 + [pltpu.SemaphoreType.DMA((3,))] + [field] * 9 + [plane] * 2,
        "pressure",
        near(got),
        obs_values.reshape(1, observed),
        obs_noise.reshape(members, observed),
        obs_var.reshape(1, observed),
        spaces=[pltpu.VMEM] + [pl.ANY] * 3,
        outs=[pl.BlockSpec(memory_space=pltpu.VMEM)] * 3,
    )
    returned = exchange(picked.reshape(members * n_obs, 1, nz))
    sums = vmem_call(
        functools.partial(sums_kernel, devices=devices),
        pltpu.VMEM((devices, 2 * held, members), jnp.float32),
        [],
        "sums",
        near(returned.reshape(members, observed)),
        near(aim),
        near(scale),
    )
    own = vmem_call(spread_kernel, pltpu.VMEM(sums.shape, jnp.float32), [], "spread", near(exchange(sums)))
    gathered = exchange(own)
    updated, predicted = vmem_call(
        functools.partial(update_kernel, devices=devices),
        [
            jax.ShapeDtypeStruct((members * block, nz), jnp.float32),
            jax.ShapeDtypeStruct((members, n_obs * nz), jnp.float32),
        ],
        [pltpu.VMEM((members, members), jnp.float32)] * 2 + [pltpu.SemaphoreType.DMA],
        "update",
        near(gathered),
        near(ensemble.reshape(members * block, nz)),
        near(returned.reshape(members, n_obs * nz)),
        outs=[pl.BlockSpec(memory_space=pltpu.VMEM), pl.BlockSpec(memory_space=pl.ANY)],
    )
    return (updated.reshape(ensemble.shape), predicted.reshape(members, 1, 1, n_obs * nz))


def local(ensemble, *rest):
    devices = lax.axis_size("member") * lax.axis_size("space")
    form = local_whole if ensemble.shape[0] % devices == 0 else local_split
    return form(ensemble, *rest)


def solution(mesh):
    in_specs = (
        P(None, "space", "member", None),
        P("space", "member", None),
        P("space", "member", None),
        P("space", "member", None),
        P(None, "space", "member", None),
        P("space", "member", None),
    )
    out_specs = (P(None, "space", "member", None), P(None, "space", "member", None))
    return jax.shard_map(local, mesh=mesh, in_specs=in_specs, out_specs=out_specs, check_vma=False)
```
